32 devices in a mesh: seq: 8 (over z, x), head: 4 (over y, core).
Axes of the slice: x: 2, y: 2, z: 4, core: 2. Of those that a mesh axis runs over, the one named last changes fastest.
Arguments:
- tokens: bfloat16 [2048, 3584], P('seq'), may hold values from -16 to 16
- length: int32 [1], replicated, may hold values from 512 to 2048
- in_gain: float32 [3584], replicated, may hold values from 0.5 to 1.5
- q_weight: bfloat16 [3584, 3584], P(None, 'head'), may hold values from -0.09375 to 0.09375
- q_bias: float32 [3584], P('head'), may hold values from -60 to 60
- k_weight: bfloat16 [3584, 512], P(None, 'head'), may hold values from -0.09375 to 0.09375
- k_bias: float32 [512], P('head'), may hold values from -60 to 60
- v_weight: bfloat16 [3584, 512], P(None, 'head'), may hold values from -0.09375 to 0.09375
- v_bias: float32 [512], P('head'), may hold values from -2 to 2
- o_weight: bfloat16 [3584, 3584], P('head'), may hold values from -0.125 to 0.125
- final_gain: float32 [3584], P('head'), may hold values from 0.5 to 1.5
Outputs:
- hidden: bfloat16 [2048, 3584], P('seq', 'head')
- embedding: float32 [3584], P('head')
The draws below stay inside these ranges and needn't reach their ends.
All inputs are finite; a program needn't handle non-finite values.
Results may differ from the reference program's by a relative error of at most 0.0075.
The reference program's roundings to bfloat16 on the way (of `normed`, `query` and `attended`) count: a program that leaves them out, or rounds other values in their place, can miss the bound.
Values may be sent and summed in bfloat16 or wider, within the bound.
A program may use at most 192 MiB of HBM per device.

```python
import jax
import jax.numpy as jnp
from jax import lax

D = 3584
HEADS = 28
KV_HEADS = 4
HEAD_DIM = 128
TOKENS = 2048


def draw_tokens(key, part):
    place = (jnp.arange(D, dtype=jnp.float32) + 0.5) / D
    tilt = jax.random.uniform(jax.random.fold_in(key, 11), (TOKENS, 1), jnp.float32, -1.0, 1.0)
    noise = jnp.clip(jax.random.normal(jax.random.fold_in(key, 12), (TOKENS, D), jnp.float32), -6.0, 6.0)
    scale = jnp.exp(tilt * 0.92 * (2.0 * place[None, :] - 1.0))
    return (noise * scale).astype(jnp.bfloat16)


def draw_k_bias(key, part):
    noise = 0.3 * jnp.clip(jax.random.normal(jax.random.fold_in(key, 1), (KV_HEADS * HEAD_DIM,), jnp.float32), -6.0, 6.0)
    return noise


def draw_q_bias(key, part):
    noise = 0.3 * jnp.clip(jax.random.normal(jax.random.fold_in(key, 2), (HEADS * HEAD_DIM,), jnp.float32), -6.0, 6.0)
    return noise


def with_spikes(array, own_key, source, target, blocks, factor):
    owner, partner = [(jnp.arange(array.shape[dim]) // (array.shape[dim] // blocks)).reshape([-1 if axis == dim else 1 for axis in range(array.ndim)]) for dim in (source, target)]
    chosen = jax.random.permutation(own_key, blocks)[partner]
    strong = (owner == chosen) | (owner == (partner + blocks // 2) % blocks)
    return jnp.where(strong, factor * array, array)


def block_levels(stream_key, extent, split, least, high):
    loudness = 1.0
    for axis_at, blocks in split:
        heights = jax.random.uniform(jax.random.fold_in(jax.random.fold_in(stream_key, 6), axis_at), (blocks,), jnp.float32, least / len(split), high / len(split))
        loudness = loudness * jnp.repeat(jnp.exp(heights), extent[axis_at] // blocks).reshape((-1,) + (1,) * (len(extent) - 1 - axis_at))
    return loudness


def bell_draw(own_key, shape, deviation, limit, pieces=(), held_as=jnp.bfloat16):
    loudness = block_levels(own_key, shape, pieces, -0.22, 0.18) if pieces else 1.0
    entries = jax.random.normal(own_key, shape, jnp.float32) * deviation * loudness
    return jnp.minimum(jnp.maximum(entries, -limit), limit).astype(held_as)


def bell_draw_with(own_key, dims, spread, most, split, heavy, held_as=jnp.bfloat16):
    entries = spread * jax.random.normal(own_key, dims, jnp.float32)
    if split:
        entries = entries * block_levels(own_key, dims, split, -0.22, 0.18)
    return jnp.clip(with_spikes(entries, jax.random.fold_in(own_key, 3), *heavy), -most, most).astype(held_as)


def setup_inputs(seed: int = 0) -> dict:
    key_of = jax.random.split(jax.random.key(seed), 12)
    return {
        "tokens": draw_tokens(jax.random.fold_in(key_of[11], 71), 0),
        "length": jax.random.randint(key_of[1], (1,), TOKENS // 4, TOKENS + 1).astype(jnp.int32),
        "in_gain": jnp.clip(1.0 + 0.1 * jax.random.normal(key_of[2], (D,), jnp.float32), 0.5, 1.5),
        "q_weight": bell_draw(key_of[3], (D, HEADS * HEAD_DIM), D ** -0.5, 0.09375, ((1, 4),)),
        "q_bias": draw_q_bias(jax.random.fold_in(key_of[11], 71), 0),
        "k_weight": bell_draw(key_of[5], (D, KV_HEADS * HEAD_DIM), D ** -0.5, 0.09375, ((1, 4),)),
        "k_bias": draw_k_bias(jax.random.fold_in(key_of[11], 71), 0),
        "v_weight": bell_draw(key_of[7], (D, KV_HEADS * HEAD_DIM), D ** -0.5, 0.09375, ((1, 4),)),
        "v_bias": bell_draw(key_of[8], (KV_HEADS * HEAD_DIM,), 0.3, 2.0, ((0, 4),), jnp.float32),
        "o_weight": bell_draw_with(key_of[9], (HEADS * HEAD_DIM, D), (HEADS * HEAD_DIM) ** -0.5, 0.125, ((0, 4),), (0, 1, 4, 2.0)),
        "final_gain": jnp.clip(1.0 + 0.1 * jax.random.normal(key_of[10], (D,), jnp.float32), 0.5, 1.5),
    }


rope_base = 1000000.0
epsilon = 1e-06

def rms_norm(inputs, gain):
    inputs = inputs.astype(jnp.float32)
    return inputs * lax.rsqrt(lax.optimization_barrier(jnp.mean(inputs * inputs, axis=-1, keepdims=True)) + epsilon) * gain

def rope_tables(positions):
    half_dim = HEAD_DIM // 2
    inverse = rope_base ** (-(jnp.arange(half_dim, dtype=jnp.float32) * 2.0) / HEAD_DIM)
    angles = positions.astype(jnp.float32)[:, None] * inverse[None, :]
    angles = jnp.concatenate([angles, angles], axis=1)
    return (jnp.cos(angles), jnp.sin(angles))

def rotate(inputs, cosine, sine):
    half_dim = HEAD_DIM // 2
    turned = jnp.concatenate([-inputs[..., half_dim:], inputs[..., :half_dim]], axis=-1)
    return inputs * cosine[:, None, :] + turned * sine[:, None, :]

def reference(tokens, length, in_gain, q_weight, q_bias, k_weight, k_bias, v_weight, v_bias, o_weight, final_gain):
    seq_len = tokens.shape[0]
    group_size = HEADS // KV_HEADS
    normed = rms_norm(tokens, in_gain).astype(jnp.bfloat16)
    cosine, sine = rope_tables(jnp.arange(seq_len, dtype=jnp.int32))
    query = jnp.dot(normed, q_weight, preferred_element_type=jnp.float32) + q_bias
    query = (rotate(query.reshape(seq_len, HEADS, HEAD_DIM), cosine, sine) * HEAD_DIM ** (-0.5)).astype(jnp.bfloat16)
    keys = jnp.dot(normed, k_weight, preferred_element_type=jnp.float32) + k_bias
    keys = rotate(keys.reshape(seq_len, KV_HEADS, HEAD_DIM), cosine, sine).astype(jnp.bfloat16)
    values = (jnp.dot(normed, v_weight, preferred_element_type=jnp.float32) + v_bias).astype(jnp.bfloat16)
    values = values.reshape(seq_len, KV_HEADS, HEAD_DIM)
    live = jnp.arange(seq_len, dtype=jnp.int32) < length[0]

    def one_head(index):
        kv_index = index // group_size
        q_head = lax.dynamic_index_in_dim(query, index, 1, keepdims=False)
        k_head = lax.dynamic_index_in_dim(keys, kv_index, 1, keepdims=False)
        v_head = lax.dynamic_index_in_dim(values, kv_index, 1, keepdims=False)
        scores = lax.dot_general(q_head, k_head, (((1,), (1,)), ((), ())), preferred_element_type=jnp.float32)
        scores = jnp.where(live[None, :], scores, -1e+30)
        top = lax.optimization_barrier(jnp.max(scores, axis=1, keepdims=True))
        weights = jnp.where(live[None, :], jnp.exp(scores - top), 0.0)
        total = lax.optimization_barrier(jnp.sum(weights, axis=1, keepdims=True))
        mixed = jnp.dot(weights.astype(jnp.bfloat16), v_head, preferred_element_type=jnp.float32)
        return (mixed / total).astype(jnp.bfloat16)
    heads_out = lax.map(one_head, jnp.arange(HEADS, dtype=jnp.int32))
    attended = jnp.transpose(heads_out, (1, 0, 2)).reshape(seq_len, HEADS * HEAD_DIM)
    hidden_full = tokens.astype(jnp.float32) + jnp.dot(attended, o_weight, preferred_element_type=jnp.float32)
    hidden = hidden_full.astype(jnp.bfloat16)
    final = rms_norm(hidden_full, final_gain)
    pooled_sum = lax.optimization_barrier(jnp.sum(jnp.where(live[:, None], final, 0.0), axis=0))
    mean = pooled_sum / length[0].astype(jnp.float32)
    embedding = mean * lax.rsqrt(jnp.mean(mean * mean) + epsilon)
    return (hidden, embedding)
```

```python
import functools

import jax
import jax.numpy as jnp
import numpy as np
from jax import lax
from jax.experimental import pallas as pl
from jax.experimental.pallas import tpu as pltpu
from jax.sharding import PartitionSpec as P

HEAD_DIM = 128
ROPE_BASE = 1000000.0
EPS = 1e-06
MESH = pl.DeviceIdType.MESH
F32 = jnp.float32
BF16 = jnp.bfloat16
LOW = -1e30


def widths(share):
    out, at = [], 0
    first = share % 256 or 256
    while at < share:
        width = first if at == 0 else 256
        out.append((1, at, width))
        at += width
    cut = out[len(out) // 2][1]
    return [(0, 0, cut), (0, cut, share - cut)] + out


def dot(a, b):
    return jnp.dot(a, b, preferred_element_type=F32)


def kernel(
    n_seq,
    n_head,
    length_hbm,
    tokens_hbm,
    gain_hbm,
    wq_hbm,
    qb_hbm,
    wk_hbm,
    kb_hbm,
    wv_hbm,
    vb_hbm,
    wo_hbm,
    fgain_hbm,
    near_hbm,
    far_hbm,
    hid_bf,
    emb_ref,
    length_ref,
    gain_1d,
    qb_1d,
    kb_1d,
    vb_1d,
    fgain_1d,
    near,
    far,
    gain_ref,
    qb_ref,
    kb_ref,
    vb_ref,
    fgain_ref,
    tok,
    normed,
    wkv,
    wq,
    wo,
    cos,
    sin,
    qt,
    kbuf,
    vbuf,
    m_ref,
    l_ref,
    acc_ref,
    att,
    hid,
    sqbuf,
    pbuf,
    wbuf,
    local_sem,
    ring_send,
    ring_recv,
    pair_send,
    pair_recv,
    cross_send,
    cross_recv,
    sq_send,
    sq_recv,
    pool_send,
    pool_recv,
    pow_send,
    pow_recv,
    *chunk_bufs,
):
    rows, width = tok.shape
    share = hid.shape[1]
    heads = qt.shape[2] // (rows // 2)
    part_rows = rows // 2
    half = n_seq // 2
    n_y = n_head // 2
    chunks = widths(share)
    psend, precv = chunk_bufs[0::5], chunk_bufs[1::5]
    pown, ysend, yrecv = chunk_bufs[2::5], chunk_bufs[3::5], chunk_bufs[4::5]
    ms = lax.axis_index("seq")
    mh = lax.axis_index("head")

    loads = [
        pltpu.make_async_copy(tokens_hbm, tok, local_sem.at[0]),
        pltpu.make_async_copy(wk_hbm, wkv.at[:, :HEAD_DIM], local_sem.at[1]),
        pltpu.make_async_copy(wv_hbm, wkv.at[:, HEAD_DIM:], local_sem.at[2]),
        pltpu.make_async_copy(wq_hbm, wq, local_sem.at[3]),
        pltpu.make_async_copy(wo_hbm, wo, local_sem.at[4]),
    ]
    smalls = [
        pltpu.make_async_copy(near_hbm, near, local_sem.at[5]),
        pltpu.make_async_copy(far_hbm.at[ms], far, local_sem.at[6]),
        pltpu.make_async_copy(gain_hbm, gain_1d, local_sem.at[7]),
        pltpu.make_async_copy(kb_hbm, kb_1d, local_sem.at[8]),
        pltpu.make_async_copy(vb_hbm, vb_1d, local_sem.at[9]),
        pltpu.make_async_copy(qb_hbm, qb_1d, local_sem.at[10]),
        pltpu.make_async_copy(fgain_hbm, fgain_1d, local_sem.at[11]),
        pltpu.make_async_copy(length_hbm, length_ref, local_sem.at[12]),
    ]
    loads[0].start()
    for small in smalls:
        small.start()
    for load in loads[1:4]:
        load.start()

    barrier = pltpu.get_barrier_semaphore()

    def greet(d, carry):
        pl.semaphore_signal(
            barrier, inc=1, device_id={"seq": lax.rem(ms + d, n_seq)}, device_id_type=MESH
        )
        return carry

    lax.fori_loop(1, n_seq, greet, 0)
    for d in range(1, n_head):
        pl.semaphore_signal(
            barrier, inc=1, device_id={"head": lax.rem(mh + d, n_head)}, device_id_type=MESH
        )

    def rope(u):
        return u * cos[...] + pltpu.roll(u, HEAD_DIM // 2, 1) * sin[...]

    for small in smalls:
        small.wait()
    limit = length_ref[0]
    for flat, row in (
        (gain_1d, gain_ref),
        (qb_1d, qb_ref),
        (kb_1d, kb_ref),
        (vb_1d, vb_ref),
        (fgain_1d, fgain_ref),
    ):
        for g in range(0, row.shape[1], HEAD_DIM):
            row[:, g : g + HEAD_DIM] = flat[g : g + HEAD_DIM].reshape(1, HEAD_DIM)

    lane = lax.broadcasted_iota(jnp.int32, (1, HEAD_DIM), 1)
    sign = jnp.where(lane < HEAD_DIM // 2, -1.0, 1.0)
    co, so = far[0, :1], far[1, :1]
    cos[...] = near[0] * co - near[1] * so
    sin[...] = (near[1] * co + near[0] * so) * sign

    loads[0].wait()
    block = 16

    def norm_block(i, carry):
        at = pl.ds(pl.multiple_of(i * block, block), block)
        x = tok[at, :].astype(F32)
        mean = jnp.sum(x * x, axis=1, keepdims=True) / width
        normed[at, :] = (x * lax.rsqrt(mean + EPS) * gain_ref[...]).astype(BF16)
        return carry

    lax.fori_loop(0, rows // block, norm_block, 0)

    loads[1].wait()
    loads[2].wait()
    kv = dot(normed[...], wkv[...])
    kbuf[ms] = rope(kv[:, :HEAD_DIM] + kb_ref[...]).astype(BF16)
    vbuf[ms] = jnp.transpose(kv[:, HEAD_DIM:] + vb_ref[...]).astype(BF16)

    q2 = lax.div(ms, 2)
    pos = q2 + (ms - 2 * q2) * (n_seq - 1 - 2 * q2)

    def slot(p):
        p = lax.rem(p + 2 * n_seq, n_seq)
        back = lax.div(p, half)
        return (1 - back) * 2 * p + back * (2 * (n_seq - 1 - p) + 1)

    ends = (slot(pos + 1), slot(pos - 1))

    def moved(way, kind, s, hops):
        sign_of = 1 if way == 0 else -1
        at = slot(pos - sign_of * hops)
        buf = vbuf if kind else kbuf
        return pltpu.make_async_remote_copy(
            src_ref=buf.at[at],
            dst_ref=buf.at[at],
            send_sem=ring_send.at[2 * way + kind, s],
            recv_sem=ring_recv.at[2 * way + kind, s],
            device_id={"seq": ends[way]},
            device_id_type=MESH,
        )

    def send(way, kind, s):
        return moved(way, kind, s, s - 1)

    def arrival(way, kind, s):
        return moved(way, kind, s, s)

    pl.semaphore_wait(barrier, n_seq + n_head - 2)
    for kind in (0, 1):
        for way in (0, 1):
            send(way, kind, 1).start()

    def put_query(h, u):
        at = pl.ds(pl.multiple_of(h * HEAD_DIM, HEAD_DIM), HEAD_DIM)
        to = pl.ds(pl.multiple_of(h * part_rows, part_rows), part_rows)
        u = rope(u + qb_ref[:, at]) * HEAD_DIM ** (-0.5)
        u = jnp.transpose(u).astype(BF16)
        qt[0, :, to] = u[:, :part_rows]
        qt[1, :, to] = u[:, part_rows:]

    loads[3].wait()
    loads[4].start()

    def query_pair(j, carry):
        at = pl.ds(pl.multiple_of(j * 2 * HEAD_DIM, 2 * HEAD_DIM), 2 * HEAD_DIM)
        u = dot(normed[...], wq[:, at])
        put_query(2 * j, u[:, :HEAD_DIM])
        put_query(2 * j + 1, u[:, HEAD_DIM:])
        return carry

    lax.fori_loop(0, heads // 2, query_pair, 0)
    if heads % 2:
        put_query(heads - 1, dot(normed[...], wq[:, (heads - 1) * HEAD_DIM :]))

    m_ref[...] = jnp.full(m_ref.shape, LOW, F32)
    l_ref[...] = jnp.zeros(l_ref.shape, F32)
    acc_ref[...] = jnp.zeros(acc_ref.shape, F32)
    lanes = heads * part_rows
    tiles = [(t, min(256, lanes - t)) for t in range(0, lanes, 256)]

    def attend(part, blocks):
        row_at = lax.broadcasted_iota(jnp.int32, (rows, 1), 0)
        live = [b * rows + row_at < limit for b in blocks]
        for t, wide in tiles:
            at = slice(t, t + wide)
            query = qt[part, :, at]
            scores = [jnp.where(ok, dot(kbuf[b], query), LOW) for b, ok in zip(blocks, live)]
            tops = [jnp.max(s, axis=0, keepdims=True) for s in scores]
            old = m_ref[part, :, at][:1]
            top = functools.reduce(jnp.maximum, tops, old)
            alpha = jnp.exp(old - top)
            total = l_ref[part, :, at][:1] * alpha
            mixed = acc_ref[part, :, at] * alpha
            for b, s in zip(blocks, scores):
                p = jnp.exp(s - top)
                total = total + jnp.sum(p, axis=0, keepdims=True)
                mixed = mixed + dot(vbuf[b], p.astype(BF16))
            m_ref[part, :, at] = jnp.broadcast_to(top, (8, wide))
            l_ref[part, :, at] = jnp.broadcast_to(total, (8, wide))
            acc_ref[part, :, at] = mixed

    def forward(s, kinds_ways):
        for kind in (0, 1):
            for way in (0, 1):
                arrival(way, kind, s).wait_recv()
                if (way, kind) in kinds_ways:
                    send(way, kind, s + 1).start()

    every = ((0, 0), (0, 1), (1, 0), (1, 1))
    last = ((0, 0), (1, 1))
    forward(1, every if half > 2 else last)
    attend(0, [ms])
    attend(0, [slot(pos - 1), slot(pos + 1)])

    def ring_step(s, carry):
        forward(s, every)
        attend(0, [slot(pos - s), slot(pos + s)])
        return carry

    if half > 3:
        lax.fori_loop(2, half - 1, ring_step, 0)
    if half > 2:
        forward(half - 1, last)
        attend(0, [slot(pos - half + 1), slot(pos + half - 1)])
    for way, kind in last:
        arrival(way, kind, half).wait_recv()
    attend(0, [slot(pos - half)])

    def finish(part):
        for h in range(heads):
            at = slice(h * part_rows, (h + 1) * part_rows)
            done = jnp.transpose(acc_ref[part, :, at] / l_ref[part, :, at][:1]).astype(BF16)
            cols = slice(h * HEAD_DIM, (h + 1) * HEAD_DIM)
            att[part * part_rows : (part + 1) * part_rows, cols] = done

    loads[4].wait()
    my = lax.div(mh, 2)
    mc = mh - 2 * my
    partner = 2 * my + 1 - mc

    def partial(part, dest, at, wide):
        cols = pl.ds(pl.multiple_of(dest * share + at, HEAD_DIM), wide)
        return dot(att[part * part_rows : (part + 1) * part_rows, :], wo[:, cols])

    def pair_copy(i):
        return pltpu.make_async_remote_copy(
            src_ref=psend[i],
            dst_ref=precv[i],
            send_sem=pair_send.at[i],
            recv_sem=pair_recv.at[i],
            device_id={"head": partner},
            device_id_type=MESH,
        )

    def cross_copy(i, d):
        return pltpu.make_async_remote_copy(
            src_ref=ysend[i].at[d - 1],
            dst_ref=yrecv[i].at[d - 1],
            send_sem=cross_send.at[i, d - 1],
            recv_sem=cross_recv.at[i, d - 1],
            device_id={"head": 2 * lax.rem(my + d, n_y) + mc},
            device_id_type=MESH,
        )

    def to_partner(i):
        part, at, wide = chunks[i]
        for y in range(n_y):
            psend[i][y] = partial(part, 2 * y + 1 - mc, at, wide).astype(BF16)
        pair_copy(i).start()
        for d in range(1, n_y):
            pown[i][d] = partial(part, 2 * lax.rem(my + d, n_y) + mc, at, wide)

    def across(i):
        pair_copy(i).wait_recv()
        for d in range(1, n_y):
            y = lax.rem(my + d, n_y)
            ysend[i][d - 1] = (pown[i][d] + precv[i][y].astype(F32)).astype(BF16)
            cross_copy(i, d).start()

    early = [i for i, c in enumerate(chunks) if c[0] == 0]
    late = [i for i, c in enumerate(chunks) if c[0] == 1]
    finish(0)
    for i in early:
        to_partner(i)
    attend(1, [0, 1])
    for i in early:
        across(i)

    def whole_step(i, carry):
        attend(1, [2 * i, 2 * i + 1])
        return carry

    lax.fori_loop(1, half, whole_step, 0)
    finish(1)
    for i in late:
        to_partner(i)
        if i > late[0]:
            across(i - 1)
    across(late[-1])
    for i, (part, at, wide) in enumerate(chunks):
        pown[i][0] = partial(part, mh, at, wide)

    squares = [None, None]
    for i, (part, at, wide) in enumerate(chunks):
        mine = pl.ds(pl.multiple_of(mh * share + at, HEAD_DIM), wide)
        band = slice(part * part_rows, (part + 1) * part_rows)
        base = tok[band, mine].astype(F32) + (pown[i][0] + precv[i][my].astype(F32))
        for d in range(1, n_y):
            cross_copy(i, d).wait_recv()
            base = base + yrecv[i][d - 1].astype(F32)
        hid[band, at : at + wide] = base
        hid_bf[band, at : at + wide] = base.astype(BF16)
        for g in range(0, wide, HEAD_DIM):
            piece = base[:, g : g + HEAD_DIM]
            more = piece * piece
            squares[part] = more if squares[part] is None else squares[part] + more
    squares = jnp.concatenate(squares, axis=0)

    def head_copy(buf, send_sems, recv_sems, d):
        return pltpu.make_async_remote_copy(
            src_ref=buf.at[mh],
            dst_ref=buf.at[mh],
            send_sem=send_sems.at[d - 1],
            recv_sem=recv_sems.at[d - 1],
            device_id={"head": lax.rem(mh + d, n_head)},
            device_id_type=MESH,
        )

    def head_arrival(buf, send_sems, recv_sems, d):
        source = lax.rem(mh + n_head - d, n_head)
        return pltpu.make_async_remote_copy(
            src_ref=buf.at[source],
            dst_ref=buf.at[source],
            send_sem=send_sems.at[d - 1],
            recv_sem=recv_sems.at[d - 1],
            device_id={"head": source},
            device_id_type=MESH,
        )

    def head_sum(buf, send_sems, recv_sems, value):
        buf[mh] = jnp.broadcast_to(value, buf.shape[1:])
        for d in range(1, n_head):
            head_copy(buf, send_sems, recv_sems, d).start()
        for d in range(1, n_head):
            head_arrival(buf, send_sems, recv_sems, d).wait_recv()
        return functools.reduce(lambda a, b: a + b, [buf[d][:1] for d in range(n_head)])

    square_row = jnp.sum(jnp.transpose(squares), axis=0, keepdims=True)
    power = head_sum(sqbuf, sq_send, sq_recv, square_row)
    place = ms * rows + lax.broadcasted_iota(jnp.int32, (1, rows), 1)
    scale = jnp.where(place < limit, lax.rsqrt(power / width + EPS), 0.0)
    scale = jnp.transpose(jnp.broadcast_to(scale, (HEAD_DIM, rows)))

    groups = pbuf.shape[1]
    sums = []
    for g in range(0, share, HEAD_DIM):
        at = slice(g, g + HEAD_DIM)
        sums.append(jnp.sum(hid[:, at] * scale, axis=0, keepdims=True) * fgain_ref[:, at])
    sums += [jnp.zeros((1, HEAD_DIM), F32)] * (groups - len(sums))
    pbuf[ms] = jnp.concatenate(sums, axis=0)

    def pool_copy(d):
        return pltpu.make_async_remote_copy(
            src_ref=pbuf.at[ms],
            dst_ref=pbuf.at[ms],
            send_sem=pool_send.at[d - 1],
            recv_sem=pool_recv.at[d - 1],
            device_id={"seq": lax.rem(ms + d, n_seq)},
            device_id_type=MESH,
        )

    def pool_start(d, carry):
        pool_copy(d).start()
        return carry

    def pool_wait(d, carry):
        source = lax.rem(ms + n_seq - d, n_seq)
        pltpu.make_async_remote_copy(
            src_ref=pbuf.at[source],
            dst_ref=pbuf.at[source],
            send_sem=pool_send.at[d - 1],
            recv_sem=pool_recv.at[d - 1],
            device_id={"seq": source},
            device_id_type=MESH,
        ).wait_recv()
        return carry

    lax.fori_loop(1, n_seq, pool_start, 0)
    lax.fori_loop(1, n_seq, pool_wait, 0)
    mean = functools.reduce(lambda a, b: a + b, [pbuf[d] for d in range(n_seq)])
    mean = mean / limit.astype(F32)
    total = head_sum(wbuf, pow_send, pow_recv, jnp.sum(mean * mean, axis=0, keepdims=True))
    pooled = mean * lax.rsqrt(jnp.sum(total, axis=1, keepdims=True) / width + EPS)
    for g in range(share // HEAD_DIM):
        emb_ref[g * HEAD_DIM : (g + 1) * HEAD_DIM] = pooled[g : g + 1].reshape(HEAD_DIM)

    def sent(s, carry):
        for way, kind in every:
            send(way, kind, s).wait_send()
        return carry

    lax.fori_loop(1, half, sent, 0)
    for way, kind in last:
        send(way, kind, half).wait_send()
    for i in range(len(chunks)):
        pair_copy(i).wait_send()
        for d in range(1, n_y):
            cross_copy(i, d).wait_send()
    for d in range(1, n_head):
        head_copy(sqbuf, sq_send, sq_recv, d).wait_send()
        head_copy(wbuf, pow_send, pow_recv, d).wait_send()

    def pool_sent(d, carry):
        pool_copy(d).wait_send()
        return carry

    lax.fori_loop(1, n_seq, pool_sent, 0)


def write_out(hidden_ref, emb_ref, hidden_hbm, emb_hbm, sems):
    copies = [
        pltpu.make_async_copy(hidden_ref, hidden_hbm, sems.at[0]),
        pltpu.make_async_copy(emb_ref, emb_hbm, sems.at[1]),
    ]
    for copy in copies:
        copy.start()
    for copy in copies:
        copy.wait()


def body(
    n_seq,
    n_head,
    tokens,
    length,
    in_gain,
    q_weight,
    q_bias,
    k_weight,
    k_bias,
    v_weight,
    v_bias,
    o_weight,
    final_gain,
):
    rows, width = tokens.shape
    share = width // n_head
    heads = q_weight.shape[1] // HEAD_DIM
    half = n_seq // 2
    n_y = n_head // 2
    inverse = ROPE_BASE ** (-(np.arange(HEAD_DIM // 2) * 2.0) / HEAD_DIM)
    inverse = np.concatenate([inverse, inverse])[None, :]
    near = np.arange(rows)[:, None] * inverse
    near = np.stack([np.cos(near), np.sin(near)]).astype(np.float32)
    far = (np.arange(n_seq) * rows)[:, None] * inverse
    far = np.stack([np.cos(far), np.sin(far)], axis=1).astype(np.float32)
    far = np.repeat(far[:, :, None, :], 8, axis=2)

    chunks = widths(share)
    groups = -(-share // (8 * HEAD_DIM)) * 8
    chunk_bufs = []
    for _, _, wide in chunks:
        chunk_bufs += [
            pltpu.VMEM((n_y, rows // 2, wide), BF16),
            pltpu.VMEM((n_y, rows // 2, wide), BF16),
            pltpu.VMEM((n_y, rows // 2, wide), F32),
            pltpu.VMEM((n_y - 1, rows // 2, wide), BF16),
            pltpu.VMEM((n_y - 1, rows // 2, wide), BF16),
        ]
    dma = pltpu.SemaphoreType.DMA
    hbm = pl.BlockSpec(memory_space=pltpu.HBM)
    vmem = pl.BlockSpec(memory_space=pltpu.VMEM)
    shapes = (
        jax.ShapeDtypeStruct((rows, share), BF16),
        jax.ShapeDtypeStruct((share,), F32),
    )
    operands = (
        length,
        tokens,
        in_gain,
        q_weight,
        q_bias,
        k_weight,
        k_bias,
        v_weight,
        v_bias,
        o_weight,
        final_gain,
        jnp.asarray(near),
        jnp.asarray(far),
    )
    hidden, embedding = pl.pallas_call(
        functools.partial(kernel, n_seq, n_head),
        out_shape=shapes,
        in_specs=[hbm] * 13,
        out_specs=(vmem, vmem),
        scratch_shapes=[
            pltpu.SMEM((1,), jnp.int32),
            pltpu.VMEM((width,), F32),
            pltpu.VMEM((heads * HEAD_DIM,), F32),
            pltpu.VMEM((HEAD_DIM,), F32),
            pltpu.VMEM((HEAD_DIM,), F32),
            pltpu.VMEM((share,), F32),
            pltpu.VMEM(near.shape, F32),
            pltpu.VMEM(far.shape[1:], F32),
            pltpu.VMEM((1, width), F32),
            pltpu.VMEM((1, heads * HEAD_DIM), F32),
            pltpu.VMEM((1, HEAD_DIM), F32),
            pltpu.VMEM((1, HEAD_DIM), F32),
            pltpu.VMEM((1, share), F32),
            pltpu.VMEM((rows, width), BF16),
            pltpu.VMEM((rows, width), BF16),
            pltpu.VMEM((width, 2 * HEAD_DIM), BF16),
            pltpu.VMEM(q_weight.shape, BF16),
            pltpu.VMEM(o_weight.shape, BF16),
            pltpu.VMEM((rows, HEAD_DIM), F32),
            pltpu.VMEM((rows, HEAD_DIM), F32),
            pltpu.VMEM((2, HEAD_DIM, heads * (rows // 2)), BF16),
            pltpu.VMEM((n_seq, rows, HEAD_DIM), BF16),
            pltpu.VMEM((n_seq, HEAD_DIM, rows), BF16),
            pltpu.VMEM((2, 8, heads * (rows // 2)), F32),
            pltpu.VMEM((2, 8, heads * (rows // 2)), F32),
            pltpu.VMEM((2, HEAD_DIM, heads * (rows // 2)), F32),
            pltpu.VMEM((rows, heads * HEAD_DIM), BF16),
            pltpu.VMEM((rows, share), F32),
            pltpu.VMEM((n_head, 8, rows), F32),
            pltpu.VMEM((n_seq, groups, HEAD_DIM), F32),
            pltpu.VMEM((n_head, 8, HEAD_DIM), F32),
            dma((13,)),
            dma((4, half + 1)),
            dma((4, half + 1)),
            dma((len(chunks),)),
            dma((len(chunks),)),
            dma((len(chunks), n_y)),
            dma((len(chunks), n_y)),
            dma((n_head,)),
            dma((n_head,)),
            dma((n_seq,)),
            dma((n_seq,)),
            dma((n_head,)),
            dma((n_head,)),
        ]
        + chunk_bufs,
        compiler_params=pltpu.CompilerParams(
            collective_id=0, has_side_effects=True, vmem_limit_bytes=48 * 1024 * 1024
        ),
    )(operands[0], *[pltpu.with_memory_space_constraint(x, pltpu.HBM) for x in operands[1:]])
    return pl.pallas_call(
        write_out,
        out_shape=shapes,
        in_specs=[vmem, vmem],
        out_specs=(hbm, hbm),
        scratch_shapes=[dma((2,))],
        compiler_params=pltpu.CompilerParams(vmem_limit_bytes=2 * 1024 * 1024),
    )(hidden, embedding)


def solution(mesh):
    in_specs = (
        P("seq", None),
        P(),
        P(),
        P(None, "head"),
        P("head"),
        P(None, "head"),
        P("head"),
        P(None, "head"),
        P("head"),
        P("head", None),
        P("head"),
    )
    out_specs = (P("seq", "head"), P("head"))
    step = functools.partial(body, mesh.shape["seq"], mesh.shape["head"])
    return jax.shard_map(step, mesh=mesh, in_specs=in_specs, out_specs=out_specs, check_vma=False)
```

```python
import functools

import jax
import jax.numpy as jnp
import numpy as np
from jax import lax
from jax.experimental import pallas as pl
from jax.experimental.pallas import tpu as pltpu
from jax.sharding import PartitionSpec as P

HEAD_DIM = 128
ROPE_BASE = 1000000.0
EPS = 1e-06
MESH = pl.DeviceIdType.MESH
F32 = jnp.float32
BF16 = jnp.bfloat16
LOW = -1e30


def widths(share):
    out, at = [], 0
    while at < share:
        width = 128 if at == 0 or share - at <= 256 else 256
        out.append((at, width))
        at += width
    return out


def dot(a, b):
    return jnp.dot(a, b, preferred_element_type=F32)


def kernel(
    n_seq,
    n_head,
    length_hbm,
    tokens_hbm,
    gain_hbm,
    wq_hbm,
    qb_hbm,
    wk_hbm,
    kb_hbm,
    wv_hbm,
    vb_hbm,
    wo_hbm,
    fgain_hbm,
    near_hbm,
    far_hbm,
    hid_bf,
    emb_ref,
    length_ref,
    gain_1d,
    qb_1d,
    kb_1d,
    vb_1d,
    fgain_1d,
    near,
    far,
    gain_ref,
    qb_ref,
    kb_ref,
    vb_ref,
    fgain_ref,
    tok,
    normed,
    wkv,
    wq,
    wo,
    cos,
    sin,
    qt,
    kbuf,
    vbuf,
    m_ref,
    acc_ref,
    att,
    hid,
    sqbuf,
    pbuf,
    wbuf,
    local_sem,
    ring_send,
    ring_recv,
    pair_send,
    pair_recv,
    cross_send,
    cross_recv,
    sq_send,
    sq_recv,
    pool_send,
    pool_recv,
    pow_send,
    pow_recv,
    *chunk_bufs,
):
    rows, width = tok.shape
    share = hid.shape[1]
    heads = qt.shape[1] // rows
    part_rows = rows // 2
    half = n_seq // 2
    n_y = n_head // 2
    chunks = widths(share)
    psend, precv = chunk_bufs[0::5], chunk_bufs[1::5]
    pown, ysend, yrecv = chunk_bufs[2::5], chunk_bufs[3::5], chunk_bufs[4::5]
    ms = lax.axis_index("seq")
    mh = lax.axis_index("head")

    def band(h):
        return pl.ds(h * part_rows, part_rows)

    tok_loads = [
        pltpu.make_async_copy(tokens_hbm.at[band(h)], tok.at[band(h)], local_sem.at[h])
        for h in (0, 1)
    ]
    kv_loads = [
        pltpu.make_async_copy(wk_hbm, wkv.at[:, :HEAD_DIM], local_sem.at[2]),
        pltpu.make_async_copy(wv_hbm, wkv.at[:, HEAD_DIM:], local_sem.at[3]),
    ]
    q_load = pltpu.make_async_copy(wq_hbm, wq, local_sem.at[4])
    o_load = pltpu.make_async_copy(wo_hbm, wo, local_sem.at[5])
    gain_load = pltpu.make_async_copy(gain_hbm, gain_1d, local_sem.at[6])
    smalls = [
        pltpu.make_async_copy(near_hbm, near, local_sem.at[7]),
        pltpu.make_async_copy(far_hbm.at[ms], far, local_sem.at[8]),
        pltpu.make_async_copy(kb_hbm, kb_1d, local_sem.at[9]),
        pltpu.make_async_copy(vb_hbm, vb_1d, local_sem.at[10]),
        pltpu.make_async_copy(qb_hbm, qb_1d, local_sem.at[11]),
        pltpu.make_async_copy(fgain_hbm, fgain_1d, local_sem.at[12]),
        pltpu.make_async_copy(length_hbm, length_ref, local_sem.at[13]),
    ]
    for load in [tok_loads[0], gain_load, *kv_loads, tok_loads[1], *smalls, q_load]:
        load.start()

    q2 = lax.div(ms, 2)
    pos = q2 + (ms - 2 * q2) * (n_seq - 1 - 2 * q2)

    def slot(p):
        p = lax.rem(p + 2 * n_seq, n_seq)
        back = lax.div(p, half)
        return (1 - back) * 2 * p + back * (2 * (n_seq - 1 - p) + 1)

    ends = (slot(pos + 1), slot(pos - 1))
    barrier = pltpu.get_barrier_semaphore()
    for end in ends:
        pl.semaphore_signal(barrier, inc=1, device_id={"seq": end}, device_id_type=MESH)
    for d in range(1, n_head):
        pl.semaphore_signal(
            barrier, inc=1, device_id={"head": lax.rem(mh + d, n_head)}, device_id_type=MESH
        )

    def spread(flat, row):
        for g in range(0, row.shape[1], HEAD_DIM):
            row[:, g : g + HEAD_DIM] = flat[g : g + HEAD_DIM].reshape(1, HEAD_DIM)

    m_ref[...] = jnp.full(m_ref.shape, LOW, F32)
    acc_ref[...] = jnp.zeros(acc_ref.shape, F32)
    ones = lax.broadcasted_iota(jnp.int32, (16, rows), 0)
    ones = jnp.where(ones == 0, 1.0, 0.0).astype(BF16)

    tok_loads[0].wait()
    gain_load.wait()
    spread(gain_1d, gain_ref)
    block = 16

    def norm_half(h):
        def step(i, carry):
            for k in (0, 1):
                at = pl.ds(pl.multiple_of(h * part_rows + (2 * i + k) * block, block), block)
                x = tok[at, :].astype(F32)
                mean = jnp.sum(x * x, axis=1, keepdims=True) / width
                normed[at, :] = (x * lax.rsqrt(mean + EPS) * gain_ref[...]).astype(BF16)
            return carry

        lax.fori_loop(0, part_rows // (2 * block), step, 0)

    def rope(u, h=None):
        at = slice(None) if h is None else band(h)
        return u * cos[at, :] + pltpu.roll(u, HEAD_DIM // 2, 1) * sin[at, :]

    def project(h):
        kv = dot(normed[band(h), :], wkv[...])
        kbuf[ms, band(h)] = rope(kv[:, :HEAD_DIM] + kb_ref[...], h).astype(BF16)
        vbuf[ms, h] = jnp.transpose(kv[:, HEAD_DIM:] + vb_ref[...]).astype(BF16)

    def moved(way, kind, h, s, hops):
        sign_of = 1 if way == 0 else -1
        at = slot(pos - sign_of * hops)
        part = vbuf.at[at, h] if kind else kbuf.at[at, band(h)]
        unit = 4 * way + 2 * kind + h
        return pltpu.make_async_remote_copy(
            src_ref=part,
            dst_ref=part,
            send_sem=ring_send.at[unit, s],
            recv_sem=ring_recv.at[unit, s],
            device_id={"seq": ends[way]},
            device_id_type=MESH,
        )

    def send(way, kind, h, s):
        return moved(way, kind, h, s, s - 1)

    def arrival(way, kind, h, s):
        return moved(way, kind, h, s, s)

    def send_own(h):
        for kind in (0, 1):
            for way in (0, 1):
                send(way, kind, h, 1).start()

    def forward(s, h, final):
        for kind in (0, 1):
            for way in (0, 1):
                arrival(way, kind, h, s).wait_recv()
                if not final or way == h:
                    send(way, kind, h, s + 1).start()

    norm_half(0)
    for small in smalls:
        small.wait()
    limit = length_ref[0]
    for flat, row in ((kb_1d, kb_ref), (vb_1d, vb_ref), (qb_1d, qb_ref), (fgain_1d, fgain_ref)):
        spread(flat, row)
    lane = lax.broadcasted_iota(jnp.int32, (1, HEAD_DIM), 1)
    sign = jnp.where(lane < HEAD_DIM // 2, -1.0, 1.0)
    co, so = far[0, :1], far[1, :1]
    cos[...] = near[0] * co - near[1] * so
    sin[...] = (near[1] * co + near[0] * so) * sign
    for load in kv_loads:
        load.wait()
    project(0)
    pl.semaphore_wait(barrier, n_head + 1)
    send_own(0)
    tok_loads[1].wait()
    norm_half(1)
    project(1)
    send_own(1)

    def put_query(h, u):
        u = rope(u + qb_ref[:, h * HEAD_DIM : (h + 1) * HEAD_DIM]) * HEAD_DIM ** (-0.5)
        qt[:, h * rows : (h + 1) * rows] = jnp.transpose(u).astype(BF16)

    def queries(first):
        last = min(first + 2, heads)
        u = dot(normed[...], wq[:, first * HEAD_DIM : last * HEAD_DIM])
        for h in range(first, last):
            put_query(h, u[:, (h - first) * HEAD_DIM : (h - first + 1) * HEAD_DIM])

    def attend(blocks, polls=()):
        row_at = lax.broadcasted_iota(jnp.int32, (rows, 1), 0)
        live = [b * rows + row_at < limit for b in blocks]
        polls = list(polls)

        def span(h):
            return slice(h * rows, (h + 1) * rows)

        def scores(h):
            return [jnp.where(ok, dot(kbuf[b], qt[:, span(h)]), LOW) for b, ok in zip(blocks, live)]

        def weigh(h, many):
            old = m_ref[:, span(h)][:1]
            top = functools.reduce(
                jnp.maximum, [jnp.max(s, axis=0, keepdims=True) for s in many], old
            )
            m_ref[:, span(h)] = jnp.broadcast_to(top, (8, rows))
            return h, jnp.exp(old - top), [jnp.exp(s - top).astype(BF16) for s in many]

        def mix(h, alpha, weights):
            new = None
            for b, p in zip(blocks, weights):
                v = jnp.concatenate([vbuf[b, 0], vbuf[b, 1]], axis=1)
                more = dot(jnp.concatenate([v, ones], axis=0), p)
                new = more if new is None else new + more
            acc_ref[:, span(h)] = acc_ref[:, span(h)] * alpha + new

        ready, held = scores(0), None
        for h in range(heads):
            after = scores(h + 1) if h + 1 < heads else None
            weighed = weigh(h, ready)
            if held is not None:
                mix(*held)
            held, ready = weighed, after
            if polls and polls[0][0] <= h:
                polls.pop(0)[1]()
        mix(*held)
        for _, poll in polls:
            poll()

    def polls(s, final):
        return [(1, lambda: forward(s, 0, final)), (4, lambda: forward(s, 1, final))]

    q_load.wait()
    o_load.start()
    queries(0)
    forward(1, 0, half == 2)
    queries(2)
    forward(1, 1, half == 2)
    for first in range(4, heads, 2):
        queries(first)
    attend([ms, slot(pos - 1), slot(pos + 1)], polls(2, half == 3))

    def ring_step(s, carry):
        attend([slot(pos - s), slot(pos + s)], polls(s + 1, False))
        return carry

    if half > 4:
        lax.fori_loop(2, half - 2, ring_step, 0)
    attend([slot(pos - half + 2), slot(pos + half - 2)], polls(half - 1, True))
    attend([slot(pos - half + 1), slot(pos + half - 1)])
    for way in (0, 1):
        for kind in (0, 1):
            arrival(way, kind, way, half).wait_recv()
    attend([slot(pos - half)])
    for h in range(heads):
        at = slice(h * rows, (h + 1) * rows)
        mixed = acc_ref[:HEAD_DIM, at] / acc_ref[HEAD_DIM : HEAD_DIM + 1, at]
        att[:, h * HEAD_DIM : (h + 1) * HEAD_DIM] = jnp.transpose(mixed).astype(BF16)

    o_load.wait()
    my = lax.div(mh, 2)
    mc = mh - 2 * my

    def far_y(d):
        return lax.rem(my + d, n_y)

    def partial(dest, at, wide):
        cols = pl.ds(pl.multiple_of(dest * share + at, HEAD_DIM), wide)
        return dot(att[...], wo[:, cols])

    def pair_copy(i, d):
        return pltpu.make_async_remote_copy(
            src_ref=psend[i].at[d],
            dst_ref=precv[i].at[d],
            send_sem=pair_send.at[i, d],
            recv_sem=pair_recv.at[i, d],
            device_id={"head": 2 * my + 1 - mc},
            device_id_type=MESH,
        )

    def cross_copy(i, d):
        return pltpu.make_async_remote_copy(
            src_ref=ysend[i].at[d - 1],
            dst_ref=yrecv[i].at[d - 1],
            send_sem=cross_send.at[i, d - 1],
            recv_sem=cross_recv.at[i, d - 1],
            device_id={"head": 2 * far_y(d) + mc},
            device_id_type=MESH,
        )

    def part_sums(i, d):
        at, wide = chunks[i]
        psend[i][d] = partial(2 * far_y(d) + 1 - mc, at, wide).astype(BF16)
        pair_copy(i, d).start()
        pown[i][d] = partial(2 * far_y(d) + mc, at, wide)

    def across(i):
        for d in range(1, n_y):
            pair_copy(i, d).wait_recv()
            ysend[i][d - 1] = (pown[i][d] + precv[i][d].astype(F32)).astype(BF16)
            cross_copy(i, d).start()

    for i in range(len(chunks)):
        for d in range(1, n_y):
            part_sums(i, d)
        if i:
            across(i - 1)
    across(len(chunks) - 1)
    for i in range(len(chunks)):
        part_sums(i, 0)

    squares = None
    for i, (at, wide) in enumerate(chunks):
        mine = pl.ds(pl.multiple_of(mh * share + at, HEAD_DIM), wide)
        pair_copy(i, 0).wait_recv()
        base = tok[:, mine].astype(F32) + (pown[i][0] + precv[i][0].astype(F32))
        for d in range(1, n_y):
            cross_copy(i, d).wait_recv()
            base = base + yrecv[i][d - 1].astype(F32)
        hid[:, at : at + wide] = base
        hid_bf[:, at : at + wide] = base.astype(BF16)
        for g in range(0, wide, HEAD_DIM):
            piece = base[:, g : g + HEAD_DIM]
            squares = piece * piece if squares is None else squares + piece * piece

    def head_copy(buf, send_sems, recv_sems, d):
        return pltpu.make_async_remote_copy(
            src_ref=buf.at[mh],
            dst_ref=buf.at[mh],
            send_sem=send_sems.at[d - 1],
            recv_sem=recv_sems.at[d - 1],
            device_id={"head": lax.rem(mh + d, n_head)},
            device_id_type=MESH,
        )

    def head_arrival(buf, send_sems, recv_sems, d):
        source = lax.rem(mh + n_head - d, n_head)
        return pltpu.make_async_remote_copy(
            src_ref=buf.at[source],
            dst_ref=buf.at[source],
            send_sem=send_sems.at[d - 1],
            recv_sem=recv_sems.at[d - 1],
            device_id={"head": source},
            device_id_type=MESH,
        )

    def head_sum(buf, send_sems, recv_sems, value):
        buf[mh] = jnp.broadcast_to(value, buf.shape[1:])
        for d in range(1, n_head):
            head_copy(buf, send_sems, recv_sems, d).start()
        for d in range(1, n_head):
            head_arrival(buf, send_sems, recv_sems, d).wait_recv()
        return functools.reduce(lambda a, b: a + b, [buf[d][:1] for d in range(n_head)])

    square_row = jnp.sum(jnp.transpose(squares), axis=0, keepdims=True)
    power = head_sum(sqbuf, sq_send, sq_recv, square_row)
    place = ms * rows + lax.broadcasted_iota(jnp.int32, (1, rows), 1)
    scale = jnp.where(place < limit, lax.rsqrt(power / width + EPS), 0.0)
    scale = jnp.transpose(jnp.broadcast_to(scale, (HEAD_DIM, rows)))

    groups = pbuf.shape[1]
    sums = []
    for g in range(0, share, HEAD_DIM):
        at = slice(g, g + HEAD_DIM)
        sums.append(jnp.sum(hid[:, at] * scale, axis=0, keepdims=True) * fgain_ref[:, at])
    sums += [jnp.zeros((1, HEAD_DIM), F32)] * (groups - len(sums))
    pbuf[ms] = jnp.concatenate(sums, axis=0)

    def pool_copy(d):
        return pltpu.make_async_remote_copy(
            src_ref=pbuf.at[ms],
            dst_ref=pbuf.at[ms],
            send_sem=pool_send.at[d - 1],
            recv_sem=pool_recv.at[d - 1],
            device_id={"seq": lax.rem(ms + d, n_seq)},
            device_id_type=MESH,
        )

    def pool_start(d, carry):
        pool_copy(d).start()
        return carry

    def pool_wait(d, carry):
        source = lax.rem(ms + n_seq - d, n_seq)
        pltpu.make_async_remote_copy(
            src_ref=pbuf.at[source],
            dst_ref=pbuf.at[source],
            send_sem=pool_send.at[d - 1],
            recv_sem=pool_recv.at[d - 1],
            device_id={"seq": source},
            device_id_type=MESH,
        ).wait_recv()
        return carry

    lax.fori_loop(1, n_seq, pool_start, 0)
    lax.fori_loop(1, n_seq, pool_wait, 0)
    mean = functools.reduce(lambda a, b: a + b, [pbuf[d] for d in range(n_seq)])
    mean = mean / limit.astype(F32)
    total = head_sum(wbuf, pow_send, pow_recv, jnp.sum(mean * mean, axis=0, keepdims=True))
    pooled = mean * lax.rsqrt(jnp.sum(total, axis=1, keepdims=True) / width + EPS)
    for g in range(share // HEAD_DIM):
        emb_ref[g * HEAD_DIM : (g + 1) * HEAD_DIM] = pooled[g : g + 1].reshape(HEAD_DIM)

    def sent(s, carry):
        for way in (0, 1):
            for kind in (0, 1):
                for h in (0, 1):
                    send(way, kind, h, s).wait_send()
        return carry

    lax.fori_loop(1, half, sent, 0)
    for way in (0, 1):
        for kind in (0, 1):
            send(way, kind, way, half).wait_send()
    for i in range(len(chunks)):
        for d in range(n_y):
            pair_copy(i, d).wait_send()
        for d in range(1, n_y):
            cross_copy(i, d).wait_send()
    for d in range(1, n_head):
        head_copy(sqbuf, sq_send, sq_recv, d).wait_send()
        head_copy(wbuf, pow_send, pow_recv, d).wait_send()

    def pool_sent(d, carry):
        pool_copy(d).wait_send()
        return carry

    lax.fori_loop(1, n_seq, pool_sent, 0)


def write_out(hidden_ref, emb_ref, hidden_hbm, emb_hbm, sems):
    copies = [
        pltpu.make_async_copy(hidden_ref, hidden_hbm, sems.at[0]),
        pltpu.make_async_copy(emb_ref, emb_hbm, sems.at[1]),
    ]
    for copy in copies:
        copy.start()
    for copy in copies:
        copy.wait()


def body(
    n_seq,
    n_head,
    tokens,
    length,
    in_gain,
    q_weight,
    q_bias,
    k_weight,
    k_bias,
    v_weight,
    v_bias,
    o_weight,
    final_gain,
):
    rows, width = tokens.shape
    share = width // n_head
    heads = q_weight.shape[1] // HEAD_DIM
    half = n_seq // 2
    n_y = n_head // 2
    inverse = ROPE_BASE ** (-(np.arange(HEAD_DIM // 2) * 2.0) / HEAD_DIM)
    inverse = np.concatenate([inverse, inverse])[None, :]
    near = np.arange(rows)[:, None] * inverse
    near = np.stack([np.cos(near), np.sin(near)]).astype(np.float32)
    far = (np.arange(n_seq) * rows)[:, None] * inverse
    far = np.stack([np.cos(far), np.sin(far)], axis=1).astype(np.float32)
    far = np.repeat(far[:, :, None, :], 8, axis=2)

    chunks = widths(share)
    groups = -(-share // (8 * HEAD_DIM)) * 8
    chunk_bufs = []
    for _, wide in chunks:
        chunk_bufs += [
            pltpu.VMEM((n_y, rows, wide), BF16),
            pltpu.VMEM((n_y, rows, wide), BF16),
            pltpu.VMEM((n_y, rows, wide), F32),
            pltpu.VMEM((n_y - 1, rows, wide), BF16),
            pltpu.VMEM((n_y - 1, rows, wide), BF16),
        ]
    dma = pltpu.SemaphoreType.DMA
    hbm = pl.BlockSpec(memory_space=pltpu.HBM)
    vmem = pl.BlockSpec(memory_space=pltpu.VMEM)
    shapes = (
        jax.ShapeDtypeStruct((rows, share), BF16),
        jax.ShapeDtypeStruct((share,), F32),
    )
    operands = (
        length,
        tokens,
        in_gain,
        q_weight,
        q_bias,
        k_weight,
        k_bias,
        v_weight,
        v_bias,
        o_weight,
        final_gain,
        jnp.asarray(near),
        jnp.asarray(far),
    )
    hidden, embedding = pl.pallas_call(
        functools.partial(kernel, n_seq, n_head),
        out_shape=shapes,
        in_specs=[hbm] * 13,
        out_specs=(vmem, vmem),
        scratch_shapes=[
            pltpu.SMEM((1,), jnp.int32),
            pltpu.VMEM((width,), F32),
            pltpu.VMEM((heads * HEAD_DIM,), F32),
            pltpu.VMEM((HEAD_DIM,), F32),
            pltpu.VMEM((HEAD_DIM,), F32),
            pltpu.VMEM((share,), F32),
            pltpu.VMEM(near.shape, F32),
            pltpu.VMEM(far.shape[1:], F32),
            pltpu.VMEM((1, width), F32),
            pltpu.VMEM((1, heads * HEAD_DIM), F32),
            pltpu.VMEM((1, HEAD_DIM), F32),
            pltpu.VMEM((1, HEAD_DIM), F32),
            pltpu.VMEM((1, share), F32),
            pltpu.VMEM((rows, width), BF16),
            pltpu.VMEM((rows, width), BF16),
            pltpu.VMEM((width, 2 * HEAD_DIM), BF16),
            pltpu.VMEM(q_weight.shape, BF16),
            pltpu.VMEM(o_weight.shape, BF16),
            pltpu.VMEM((rows, HEAD_DIM), F32),
            pltpu.VMEM((rows, HEAD_DIM), F32),
            pltpu.VMEM((HEAD_DIM, heads * rows), BF16),
            pltpu.VMEM((n_seq, rows, HEAD_DIM), BF16),
            pltpu.VMEM((n_seq, 2, HEAD_DIM, rows // 2), BF16),
            pltpu.VMEM((8, heads * rows), F32),
            pltpu.VMEM((HEAD_DIM + 16, heads * rows), F32),
            pltpu.VMEM((rows, heads * HEAD_DIM), BF16),
            pltpu.VMEM((rows, share), F32),
            pltpu.VMEM((n_head, 8, rows), F32),
            pltpu.VMEM((n_seq, groups, HEAD_DIM), F32),
            pltpu.VMEM((n_head, 8, HEAD_DIM), F32),
            dma((14,)),
            dma((8, half + 1)),
            dma((8, half + 1)),
            dma((len(chunks), n_y)),
            dma((len(chunks), n_y)),
            dma((len(chunks), n_y)),
            dma((len(chunks), n_y)),
            dma((n_head,)),
            dma((n_head,)),
            dma((n_seq,)),
            dma((n_seq,)),
            dma((n_head,)),
            dma((n_head,)),
        ]
        + chunk_bufs,
        compiler_params=pltpu.CompilerParams(
            collective_id=0, has_side_effects=True, vmem_limit_bytes=48 * 1024 * 1024
        ),
    )(operands[0], *[pltpu.with_memory_space_constraint(x, pltpu.HBM) for x in operands[1:]])
    return pl.pallas_call(
        write_out,
        out_shape=shapes,
        in_specs=[vmem, vmem],
        out_specs=(hbm, hbm),
        scratch_shapes=[dma((2,))],
        compiler_params=pltpu.CompilerParams(vmem_limit_bytes=2 * 1024 * 1024),
    )(hidden, embedding)


def solution(mesh):
    in_specs = (
        P("seq", None),
        P(),
        P(),
        P(None, "head"),
        P("head"),
        P(None, "head"),
        P("head"),
        P(None, "head"),
        P("head"),
        P("head", None),
        P("head"),
    )
    out_specs = (P("seq", "head"), P("head"))
    step = functools.partial(body, mesh.shape["seq"], mesh.shape["head"])
    return jax.shard_map(step, mesh=mesh, in_specs=in_specs, out_specs=out_specs, check_vma=False)
```

```python
import functools

import jax
import jax.numpy as jnp
import numpy as np
from jax import lax
from jax.experimental import pallas as pl
from jax.experimental.pallas import tpu as pltpu
from jax.sharding import PartitionSpec as P

HEAD_DIM = 128
ROPE_BASE = 1000000.0
EPS = 1e-06
MESH = pl.DeviceIdType.MESH
F32 = jnp.float32
BF16 = jnp.bfloat16
LOW = -1e30
SUBS = 1


def widths(share):
    out, at = [], 0
    while at < share:
        width = 128 if at == 0 or share - at <= 256 else 256
        out.append((at, width))
        at += width
    return out


def dot(a, b):
    return jnp.dot(a, b, preferred_element_type=F32)


def kernel(
    n_seq,
    n_head,
    length_hbm,
    tokens_hbm,
    gain_hbm,
    wq_hbm,
    qb_hbm,
    wk_hbm,
    kb_hbm,
    wv_hbm,
    vb_hbm,
    wo_hbm,
    fgain_hbm,
    near_hbm,
    far_hbm,
    hid_bf,
    emb_ref,
    length_ref,
    gain_1d,
    qb_1d,
    kb_1d,
    vb_1d,
    fgain_1d,
    near,
    far,
    gain_ref,
    qb_ref,
    kb_ref,
    vb_ref,
    fgain_ref,
    tok,
    normed,
    wkv,
    wq,
    wo,
    cos,
    sin,
    qt,
    kbuf,
    vbuf,
    m_ref,
    acc_ref,
    att,
    hid,
    psend,
    precv,
    pown,
    ysend,
    yrecv,
    sqbuf,
    pbuf,
    wbuf,
    local_sem,
    ring_send,
    ring_recv,
    pair_send,
    pair_recv,
    cross_send,
    cross_recv,
    sq_sem,
    pool_sem,
    pow_sem,
):
    rows, width = tok.shape
    share = hid.shape[1]
    heads = qt.shape[1] // rows
    part_rows = rows // 2
    half = n_seq // 2
    n_y = n_head // 2
    chunks = widths(share)
    ms = lax.axis_index("seq")
    mh = lax.axis_index("head")

    def band(h):
        return pl.ds(h * part_rows, part_rows)

    tok_loads = [
        pltpu.make_async_copy(tokens_hbm.at[band(h)], tok.at[band(h)], local_sem.at[h])
        for h in (0, 1)
    ]
    kv_loads = [
        pltpu.make_async_copy(wk_hbm, wkv.at[:, :HEAD_DIM], local_sem.at[2]),
        pltpu.make_async_copy(wv_hbm, wkv.at[:, HEAD_DIM:], local_sem.at[3]),
    ]
    q_load = pltpu.make_async_copy(wq_hbm, wq, local_sem.at[4])
    o_load = pltpu.make_async_copy(wo_hbm, wo, local_sem.at[5])
    gain_load = pltpu.make_async_copy(gain_hbm, gain_1d, local_sem.at[6])
    smalls = [
        pltpu.make_async_copy(near_hbm, near, local_sem.at[7]),
        pltpu.make_async_copy(far_hbm.at[ms], far, local_sem.at[8]),
        pltpu.make_async_copy(kb_hbm, kb_1d, local_sem.at[9]),
        pltpu.make_async_copy(vb_hbm, vb_1d, local_sem.at[10]),
        pltpu.make_async_copy(qb_hbm, qb_1d, local_sem.at[11]),
        pltpu.make_async_copy(fgain_hbm, fgain_1d, local_sem.at[12]),
        pltpu.make_async_copy(length_hbm, length_ref, local_sem.at[13]),
    ]
    for load in [tok_loads[0], gain_load, *kv_loads, tok_loads[1], *smalls, q_load]:
        load.start()

    q2 = lax.div(ms, 2)
    pos = q2 + (ms - 2 * q2) * (n_seq - 1 - 2 * q2)

    def slot(p):
        p = lax.rem(p + 2 * n_seq, n_seq)
        back = lax.div(p, half)
        return (1 - back) * 2 * p + back * (2 * (n_seq - 1 - p) + 1)

    ends = (slot(pos + 1), slot(pos - 1))
    barrier = pltpu.get_barrier_semaphore()
    for end in ends:
        pl.semaphore_signal(barrier, inc=1, device_id={"seq": end}, device_id_type=MESH)
    for d in range(1, n_head):
        pl.semaphore_signal(
            barrier, inc=1, device_id={"head": lax.rem(mh + d, n_head)}, device_id_type=MESH
        )

    def spread(flat, row):
        for g in range(0, row.shape[1], HEAD_DIM):
            row[:, g : g + HEAD_DIM] = flat[g : g + HEAD_DIM].reshape(1, HEAD_DIM)

    m_ref[...] = jnp.full(m_ref.shape, LOW, F32)
    acc_ref[...] = jnp.zeros(acc_ref.shape, F32)
    ones = lax.broadcasted_iota(jnp.int32, (16, rows), 0)
    ones = jnp.where(ones == 0, 1.0, 0.0).astype(BF16)

    tok_loads[0].wait()
    gain_load.wait()
    spread(gain_1d, gain_ref)
    block = 16

    def norm_half(h):
        def step(i, carry):
            for k in range(4):
                at = pl.ds(pl.multiple_of(h * part_rows + (4 * i + k) * block, block), block)
                x = tok[at, :].astype(F32)
                mean = jnp.sum(x * x, axis=1, keepdims=True) / width
                normed[at, :] = (x * lax.rsqrt(mean + EPS) * gain_ref[...]).astype(BF16)
            return carry

        lax.fori_loop(0, part_rows // (4 * block), step, 0)

    def rope(u, h=None):
        at = slice(None) if h is None else band(h)
        return u * cos[at, :] + pltpu.roll(u, HEAD_DIM // 2, 1) * sin[at, :]

    def project(h):
        mid = width // 512 * 256
        kv = dot(normed[band(h), :mid], wkv[:mid]) + dot(normed[band(h), mid:], wkv[mid:])
        kbuf[ms, band(h)] = rope(kv[:, :HEAD_DIM] + kb_ref[...], h).astype(BF16)
        vbuf[ms, h] = jnp.transpose(kv[:, HEAD_DIM:] + vb_ref[...]).astype(BF16)

    def moved(way, turn, sub, kind, s, hops):
        at = slot(pos - hops if way == 0 else pos + hops)
        first, count = (way ^ turn) * part_rows, part_rows // SUBS
        if kind:
            part = vbuf.at[at, way ^ turn, pl.ds(sub * (HEAD_DIM // SUBS), HEAD_DIM // SUBS)]
        else:
            part = kbuf.at[at, pl.ds(first + sub * count, count)]
        unit = (((s - 1) * 2 + turn) * 2 + way) * 2 * SUBS + sub * 2 + kind
        return pltpu.make_async_remote_copy(
            src_ref=part,
            dst_ref=part,
            send_sem=ring_send.at[kind],
            recv_sem=ring_recv.at[unit],
            device_id={"seq": ends[way]},
            device_id_type=MESH,
        )

    def send(way, turn, sub, kind, s):
        return moved(way, turn, sub, kind, s, s - 1)

    def arrival(way, turn, sub, kind, s):
        return moved(way, turn, sub, kind, s, s)

    def send_own(way, turn):
        for kind in (0, 1):
            for sub in range(SUBS):
                send(way, turn, sub, kind, 1).start()

    def forward(s, turn, go_on=True):
        for kind in (0, 1):
            for sub in range(SUBS):
                for way in (0, 1):
                    arrival(way, turn, sub, kind, s).wait_recv()
                    if go_on:
                        send(way, turn, sub, kind, s + 1).start()

    norm_half(0)
    tok_loads[1].wait()
    norm_half(1)
    for small in smalls:
        small.wait()
    limit = length_ref[0]
    for flat, row in ((kb_1d, kb_ref), (vb_1d, vb_ref), (qb_1d, qb_ref), (fgain_1d, fgain_ref)):
        spread(flat, row)
    lane = lax.broadcasted_iota(jnp.int32, (1, HEAD_DIM), 1)
    sign = jnp.where(lane < HEAD_DIM // 2, -1.0, 1.0)
    co, so = far[0, :1], far[1, :1]
    cos[...] = near[0] * co - near[1] * so
    sin[...] = (near[1] * co + near[0] * so) * sign
    for load in kv_loads:
        load.wait()
    project(0)
    pl.semaphore_wait(barrier, n_head + 1)
    send_own(0, 0)
    project(1)
    send_own(1, 0)
    send_own(0, 1)
    send_own(1, 1)

    def put_query(h, u):
        u = rope(u + qb_ref[:, h * HEAD_DIM : (h + 1) * HEAD_DIM]) * HEAD_DIM ** (-0.5)
        qt[:, h * rows : (h + 1) * rows] = jnp.transpose(u).astype(BF16)

    def queries(first):
        last = min(first + 4, heads)
        u = dot(normed[...], wq[:, first * HEAD_DIM : last * HEAD_DIM])
        for h in range(first, last):
            put_query(h, u[:, (h - first) * HEAD_DIM : (h - first + 1) * HEAD_DIM])

    def attend(blocks, poll=None, last=False):
        row_at = lax.broadcasted_iota(jnp.int32, (part_rows, 1), 0)
        live = [
            jnp.concatenate([b * rows + h * part_rows + row_at for b, h in block], axis=0) < limit
            for block in blocks
        ]

        def keys(block):
            parts = [kbuf[b, h * part_rows : (h + 1) * part_rows] for b, h in block]
            return jnp.concatenate(parts, axis=0)

        def values(block):
            return jnp.concatenate([vbuf[b, h] for b, h in block], axis=1)

        def span(h):
            return slice(h * rows, (h + 1) * rows)

        def scores(h):
            return [
                jnp.where(ok, dot(keys(block), qt[:, span(h)]), LOW)
                for block, ok in zip(blocks, live)
            ]

        def weigh(h, many):
            old = m_ref[:, span(h)][:1]
            top = functools.reduce(
                jnp.maximum, [jnp.max(s, axis=0, keepdims=True) for s in many], old
            )
            m_ref[:, span(h)] = jnp.broadcast_to(top, (8, rows))
            return h, jnp.exp(old - top), [jnp.exp(s - top).astype(BF16) for s in many]

        def mix(h, alpha, weights):
            new = None
            for block, p in zip(blocks, weights):
                more = dot(jnp.concatenate([values(block), ones], axis=0), p)
                new = more if new is None else new + more
            new = acc_ref[:, span(h)] * alpha + new
            if last:
                done = new[:HEAD_DIM] / new[HEAD_DIM : HEAD_DIM + 1]
                att[:, h * HEAD_DIM : (h + 1) * HEAD_DIM] = jnp.transpose(done).astype(BF16)
            else:
                acc_ref[:, span(h)] = new

        ready, held = scores(0), None
        for h in range(heads):
            after = scores(h + 1) if h + 1 < heads else None
            weighed = weigh(h, ready)
            if held is not None:
                mix(*held)
            held, ready = weighed, after
            if poll and h == heads // 2:
                poll()
        mix(*held)

    def whole(at):
        return ((at, 0), (at, 1))

    def pair(s):
        return [whole(slot(pos - s)), whole(slot(pos + s))]

    def cross_half(s, turn):
        return [((slot(pos - s), turn), (slot(pos + s), 1 - turn))]

    q_load.wait()
    o_load.start()
    for first in range(0, heads, 4):
        queries(first)
    forward(1, 0)
    attend([whole(ms)])
    forward(1, 1)

    def ring_step(s, carry):
        attend(pair(s), lambda: forward(s + 1, 0))
        forward(s + 1, 1)
        return carry

    if half > 4:
        lax.fori_loop(1, half - 3, ring_step, 0)
    ring_step(half - 3, 0)
    attend(pair(half - 2), lambda: forward(half - 1, 0))
    forward(half - 1, 1, False)
    attend(pair(half - 1))
    forward(half, 0, False)
    attend(cross_half(half, 0), last=True)
    o_load.wait()
    my = lax.div(mh, 2)
    mc = mh - 2 * my
    partner = {"head": 2 * my + 1 - mc}

    def far_y(d):
        return lax.rem(my + d, n_y)

    def partial(dest, at, wide):
        cols = pl.ds(pl.multiple_of(dest * share + at, HEAD_DIM), wide)
        return dot(att[...], wo[:, cols])

    def place(i):
        at, wide = chunks[i]
        return slice(at, at + wide)

    def pair_copy(i, d):
        return pltpu.make_async_remote_copy(
            src_ref=psend.at[d, :, place(i)],
            dst_ref=precv.at[d, :, place(i)],
            send_sem=pair_send.at[0],
            recv_sem=pair_recv.at[i, d],
            device_id=partner,
            device_id_type=MESH,
        )

    def cross_copy(i, d):
        return pltpu.make_async_remote_copy(
            src_ref=ysend.at[d - 1, :, place(i)],
            dst_ref=yrecv.at[d - 1, :, place(i)],
            send_sem=cross_send.at[0],
            recv_sem=cross_recv.at[i, d - 1],
            device_id={"head": 2 * far_y(d) + mc},
            device_id_type=MESH,
        )

    def part_sums(i, d):
        at, wide = chunks[i]
        psend[d, :, place(i)] = partial(2 * far_y(d) + 1 - mc, at, wide).astype(BF16)
        pair_copy(i, d).start()
        pown[d, :, place(i)] = partial(2 * far_y(d) + mc, at, wide)

    def across(i):
        for d in range(1, n_y):
            pair_copy(i, d).wait_recv()
            total = pown[d, :, place(i)] + precv[d, :, place(i)].astype(F32)
            ysend[d - 1, :, place(i)] = total.astype(BF16)
            cross_copy(i, d).start()

    @pl.when(mc == 0)
    def _():
        for i in range(len(chunks)):
            for d in range(1, n_y):
                part_sums(i, d)
            across(i)

    @pl.when(mc == 1)
    def _():
        for i in range(len(chunks)):
            for d in range(1, n_y):
                part_sums(i, d)
        for i in range(len(chunks)):
            across(i)

    for i in range(len(chunks)):
        part_sums(i, 0)

    squares = None
    for i, (at, wide) in enumerate(chunks):
        mine = pl.ds(pl.multiple_of(mh * share + at, HEAD_DIM), wide)
        pair_copy(i, 0).wait_recv()
        base = tok[:, mine].astype(F32) + (pown[0, :, place(i)] + precv[0, :, place(i)].astype(F32))
        for d in range(1, n_y):
            cross_copy(i, d).wait_recv()
            base = base + yrecv[d - 1, :, place(i)].astype(F32)
        hid[:, at : at + wide] = base
        hid_bf[:, at : at + wide] = base.astype(BF16)
        for g in range(0, wide, HEAD_DIM):
            piece = base[:, g : g + HEAD_DIM]
            squares = piece * piece if squares is None else squares + piece * piece

    def exchange(buf, axis, me, n, sems):
        def copy(d, slot_at):
            return pltpu.make_async_remote_copy(
                src_ref=buf.at[slot_at],
                dst_ref=buf.at[slot_at],
                send_sem=sems.at[0],
                recv_sem=sems.at[1],
                device_id={axis: lax.rem(me + d, n)},
                device_id_type=MESH,
            )

        for d in range(n - 1, 0, -1):
            copy(d, me).start()
        part = buf.at[pl.ds(0, n - 1)]
        pltpu.make_async_remote_copy(
            src_ref=part,
            dst_ref=part,
            send_sem=sems.at[0],
            recv_sem=sems.at[1],
            device_id=partner,
            device_id_type=MESH,
        ).wait_recv()

    def head_sum(buf, sems, value):
        buf[mh] = jnp.broadcast_to(value, buf.shape[1:])
        exchange(buf, "head", mh, n_head, sems)
        return functools.reduce(lambda a, b: a + b, [buf[d][:1] for d in range(n_head)])

    square_row = jnp.sum(jnp.transpose(squares), axis=0, keepdims=True)
    power = head_sum(sqbuf, sq_sem, square_row)
    where = ms * rows + lax.broadcasted_iota(jnp.int32, (1, rows), 1)
    scale = jnp.where(where < limit, lax.rsqrt(power / width + EPS), 0.0)
    scale = jnp.transpose(jnp.broadcast_to(scale, (HEAD_DIM, rows)))

    groups = pbuf.shape[1]
    sums = []
    for g in range(0, share, HEAD_DIM):
        at = slice(g, g + HEAD_DIM)
        sums.append(jnp.sum(hid[:, at] * scale, axis=0, keepdims=True) * fgain_ref[:, at])
    sums += [jnp.zeros((1, HEAD_DIM), F32)] * (groups - len(sums))
    pbuf[ms] = jnp.concatenate(sums, axis=0)

    exchange(pbuf, "seq", ms, n_seq, pool_sem)
    mean = functools.reduce(lambda a, b: a + b, [pbuf[d] for d in range(n_seq)])
    mean = mean / limit.astype(F32)
    total = head_sum(wbuf, pow_sem, jnp.sum(mean * mean, axis=0, keepdims=True))
    pooled = mean * lax.rsqrt(jnp.sum(total, axis=1, keepdims=True) / width + EPS)
    for g in range(share // HEAD_DIM):
        emb_ref[g * HEAD_DIM : (g + 1) * HEAD_DIM] = pooled[g : g + 1].reshape(HEAD_DIM)

    def all_sent(ref, sems, n):
        part = ref.at[pl.ds(0, n)]
        pltpu.make_async_remote_copy(
            src_ref=part,
            dst_ref=part,
            send_sem=sems.at[0],
            recv_sem=sems.at[0],
            device_id=partner,
            device_id_type=MESH,
        ).wait_send()

    all_sent(kbuf, ring_send.at[pl.ds(0, 1)], n_seq - 1)
    all_sent(vbuf, ring_send.at[pl.ds(1, 1)], n_seq - 1)
    all_sent(psend, pair_send, n_y)
    all_sent(ysend, cross_send, n_y - 1)
    all_sent(sqbuf, sq_sem, n_head - 1)
    all_sent(pbuf, pool_sem, n_seq - 1)
    all_sent(wbuf, pow_sem, n_head - 1)


def write_out(hidden_ref, emb_ref, hidden_hbm, emb_hbm, sems):
    copies = [
        pltpu.make_async_copy(hidden_ref, hidden_hbm, sems.at[0]),
        pltpu.make_async_copy(emb_ref, emb_hbm, sems.at[1]),
    ]
    for copy in copies:
        copy.start()
    for copy in copies:
        copy.wait()


def body(
    n_seq,
    n_head,
    tokens,
    length,
    in_gain,
    q_weight,
    q_bias,
    k_weight,
    k_bias,
    v_weight,
    v_bias,
    o_weight,
    final_gain,
):
    rows, width = tokens.shape
    share = width // n_head
    heads = q_weight.shape[1] // HEAD_DIM
    half = n_seq // 2
    n_y = n_head // 2
    inverse = ROPE_BASE ** (-(np.arange(HEAD_DIM // 2) * 2.0) / HEAD_DIM)
    inverse = np.concatenate([inverse, inverse])[None, :]
    near = np.arange(rows)[:, None] * inverse
    near = np.stack([np.cos(near), np.sin(near)]).astype(np.float32)
    far = (np.arange(n_seq) * rows)[:, None] * inverse
    far = np.stack([np.cos(far), np.sin(far)], axis=1).astype(np.float32)
    far = np.repeat(far[:, :, None, :], 8, axis=2)

    chunks = widths(share)
    groups = -(-share // (8 * HEAD_DIM)) * 8
    dma = pltpu.SemaphoreType.DMA
    hbm = pl.BlockSpec(memory_space=pltpu.HBM)
    vmem = pl.BlockSpec(memory_space=pltpu.VMEM)
    shapes = (
        jax.ShapeDtypeStruct((rows, share), BF16),
        jax.ShapeDtypeStruct((share,), F32),
    )
    operands = (
        length,
        tokens,
        in_gain,
        q_weight,
        q_bias,
        k_weight,
        k_bias,
        v_weight,
        v_bias,
        o_weight,
        final_gain,
        jnp.asarray(near),
        jnp.asarray(far),
    )
    hidden, embedding = pl.pallas_call(
        functools.partial(kernel, n_seq, n_head),
        out_shape=shapes,
        in_specs=[hbm] * 13,
        out_specs=(vmem, vmem),
        scratch_shapes=[
            pltpu.SMEM((1,), jnp.int32),
            pltpu.VMEM((width,), F32),
            pltpu.VMEM((heads * HEAD_DIM,), F32),
            pltpu.VMEM((HEAD_DIM,), F32),
            pltpu.VMEM((HEAD_DIM,), F32),
            pltpu.VMEM((share,), F32),
            pltpu.VMEM(near.shape, F32),
            pltpu.VMEM(far.shape[1:], F32),
            pltpu.VMEM((1, width), F32),
            pltpu.VMEM((1, heads * HEAD_DIM), F32),
            pltpu.VMEM((1, HEAD_DIM), F32),
            pltpu.VMEM((1, HEAD_DIM), F32),
            pltpu.VMEM((1, share), F32),
            pltpu.VMEM((rows, width), BF16),
            pltpu.VMEM((rows, width), BF16),
            pltpu.VMEM((width, 2 * HEAD_DIM), BF16),
            pltpu.VMEM(q_weight.shape, BF16),
            pltpu.VMEM(o_weight.shape, BF16),
            pltpu.VMEM((rows, HEAD_DIM), F32),
            pltpu.VMEM((rows, HEAD_DIM), F32),
            pltpu.VMEM((HEAD_DIM, heads * rows), BF16),
            pltpu.VMEM((n_seq, rows, HEAD_DIM), BF16),
            pltpu.VMEM((n_seq, 2, HEAD_DIM, rows // 2), BF16),
            pltpu.VMEM((8, heads * rows), F32),
            pltpu.VMEM((HEAD_DIM + 16, heads * rows), F32),
            pltpu.VMEM((rows, heads * HEAD_DIM), BF16),
            pltpu.VMEM((rows, share), F32),
            pltpu.VMEM((n_y, rows, share), BF16),
            pltpu.VMEM((n_y, rows, share), BF16),
            pltpu.VMEM((n_y, rows, share), F32),
            pltpu.VMEM((n_y - 1, rows, share), BF16),
            pltpu.VMEM((n_y - 1, rows, share), BF16),
            pltpu.VMEM((n_head, 8, rows), F32),
            pltpu.VMEM((n_seq, groups, HEAD_DIM), F32),
            pltpu.VMEM((n_head, 8, HEAD_DIM), F32),
            dma((14,)),
            dma((2,)),
            dma((SUBS * (8 * half - 4),)),
            dma((1,)),
            dma((len(chunks), n_y)),
            dma((1,)),
            dma((len(chunks), n_y - 1)),
            dma((2,)),
            dma((2,)),
            dma((2,)),
        ],
        compiler_params=pltpu.CompilerParams(
            collective_id=0, has_side_effects=True, vmem_limit_bytes=48 * 1024 * 1024
        ),
    )(operands[0], *[pltpu.with_memory_space_constraint(x, pltpu.HBM) for x in operands[1:]])
    return pl.pallas_call(
        write_out,
        out_shape=shapes,
        in_specs=[vmem, vmem],
        out_specs=(hbm, hbm),
        scratch_shapes=[dma((2,))],
        compiler_params=pltpu.CompilerParams(vmem_limit_bytes=2 * 1024 * 1024),
    )(hidden, embedding)


def solution(mesh):
    in_specs = (
        P("seq", None),
        P(),
        P(),
        P(None, "head"),
        P("head"),
        P(None, "head"),
        P("head"),
        P(None, "head"),
        P("head"),
        P("head", None),
        P("head"),
    )
    out_specs = (P("seq", "head"), P("head"))
    step = functools.partial(body, mesh.shape["seq"], mesh.shape["head"])
    return jax.shard_map(step, mesh=mesh, in_specs=in_specs, out_specs=out_specs, check_vma=False)
```

```python
import functools

import jax
import jax.numpy as jnp
import numpy as np
from jax import lax
from jax.experimental import pallas as pl
from jax.experimental.pallas import tpu as pltpu
from jax.sharding import PartitionSpec as P

HEAD_DIM = 128
ROPE_BASE = 1000000.0
EPS = 1e-06
MESH = pl.DeviceIdType.MESH
F32 = jnp.float32
BF16 = jnp.bfloat16
LOW = -1e30
SUBS = 1
GROUP = 4


def widths(share):
    out, at = [], 0
    while at < share:
        width = 128 if at == 0 or share - at <= 256 else 256
        out.append((at, width))
        at += width
    return out


def dot(a, b):
    return jnp.dot(a, b, preferred_element_type=F32)


def kernel(
    n_seq,
    n_head,
    length_hbm,
    tokens_hbm,
    gain_hbm,
    wq_hbm,
    qb_hbm,
    wk_hbm,
    kb_hbm,
    wv_hbm,
    vb_hbm,
    wo_hbm,
    fgain_hbm,
    near_hbm,
    far_hbm,
    hid_bf,
    emb_ref,
    length_ref,
    gain_1d,
    qb_1d,
    kb_1d,
    vb_1d,
    fgain_1d,
    near,
    far,
    gain_ref,
    qb_ref,
    kb_ref,
    vb_ref,
    fgain_ref,
    tok,
    normed,
    wkv,
    wq,
    wo,
    cos,
    sin,
    qt,
    kbuf,
    vbuf,
    m_ref,
    acc_ref,
    att,
    hid,
    psend,
    precv,
    pown,
    ysend,
    yrecv,
    sqbuf,
    pbuf,
    wbuf,
    local_sem,
    ring_send,
    ring_recv,
    pair_send,
    pair_recv,
    cross_send,
    cross_recv,
    sq_sem,
    pool_sem,
    pow_sem,
):
    rows, width = tok.shape
    share = hid.shape[1]
    heads = qt.shape[1] // rows
    part_rows = rows // 2
    half = n_seq // 2
    n_y = n_head // 2
    chunks = widths(share)
    ms = lax.axis_index("seq")
    mh = lax.axis_index("head")

    def band(h):
        return pl.ds(h * part_rows, part_rows)

    tok_loads = [
        pltpu.make_async_copy(tokens_hbm.at[band(h)], tok.at[band(h)], local_sem.at[h])
        for h in (0, 1)
    ]
    kv_loads = [
        pltpu.make_async_copy(wk_hbm, wkv.at[:, :HEAD_DIM], local_sem.at[2]),
        pltpu.make_async_copy(wv_hbm, wkv.at[:, HEAD_DIM:], local_sem.at[3]),
    ]
    q_load = pltpu.make_async_copy(wq_hbm, wq, local_sem.at[4])
    o_load = pltpu.make_async_copy(wo_hbm, wo, local_sem.at[5])
    gain_load = pltpu.make_async_copy(gain_hbm, gain_1d, local_sem.at[6])
    smalls = [
        pltpu.make_async_copy(near_hbm, near, local_sem.at[7]),
        pltpu.make_async_copy(far_hbm.at[ms], far, local_sem.at[8]),
        pltpu.make_async_copy(kb_hbm, kb_1d, local_sem.at[9]),
        pltpu.make_async_copy(vb_hbm, vb_1d, local_sem.at[10]),
        pltpu.make_async_copy(qb_hbm, qb_1d, local_sem.at[11]),
        pltpu.make_async_copy(fgain_hbm, fgain_1d, local_sem.at[12]),
        pltpu.make_async_copy(length_hbm, length_ref, local_sem.at[13]),
    ]
    for load in [tok_loads[0], gain_load, tok_loads[1], *kv_loads, *smalls, q_load]:
        load.start()

    q2 = lax.div(ms, 2)
    pos = q2 + (ms - 2 * q2) * (n_seq - 1 - 2 * q2)

    def slot(p):
        p = lax.rem(p + 2 * n_seq, n_seq)
        back = lax.div(p, half)
        return (1 - back) * 2 * p + back * (2 * (n_seq - 1 - p) + 1)

    ends = (slot(pos + 1), slot(pos - 1))
    my = lax.div(mh, 2)
    mc = mh - 2 * my
    partner = {"head": 2 * my + 1 - mc}
    barrier = pltpu.get_barrier_semaphore()
    for end in ends:
        pl.semaphore_signal(barrier, inc=1, device_id={"seq": end}, device_id_type=MESH)
    for d in range(1, n_head):
        pl.semaphore_signal(
            barrier, inc=1, device_id={"head": lax.rem(mh + d, n_head)}, device_id_type=MESH
        )

    def spread(flat, row):
        for g in range(0, row.shape[1], HEAD_DIM):
            row[:, g : g + HEAD_DIM] = flat[g : g + HEAD_DIM].reshape(1, HEAD_DIM)

    m_ref[...] = jnp.full(m_ref.shape, LOW, F32)
    acc_ref[...] = jnp.zeros(acc_ref.shape, F32)
    ones = lax.broadcasted_iota(jnp.int32, (16, rows), 0)
    ones = jnp.where(ones == 0, 1.0, 0.0).astype(BF16)

    tok_loads[0].wait()
    gain_load.wait()
    spread(gain_1d, gain_ref)
    block = 16

    def norm_half(h):
        def step(i, carry):
            for k in range(4):
                at = pl.ds(pl.multiple_of(h * part_rows + (4 * i + k) * block, block), block)
                x = tok[at, :].astype(F32)
                mean = jnp.sum(x * x, axis=1, keepdims=True) / width
                normed[at, :] = (x * lax.rsqrt(mean + EPS) * gain_ref[...]).astype(BF16)
            return carry

        lax.fori_loop(0, part_rows // (4 * block), step, 0)

    def rope(u, h=None):
        at = slice(None) if h is None else band(h)
        return u * cos[at, :] + pltpu.roll(u, HEAD_DIM // 2, 1) * sin[at, :]

    def project(h):
        mid = width // 512 * 256
        kv = dot(normed[band(h), :mid], wkv[:mid]) + dot(normed[band(h), mid:], wkv[mid:])
        kbuf[ms, band(h)] = rope(kv[:, :HEAD_DIM] + kb_ref[...], h).astype(BF16)
        vbuf[ms, h] = jnp.transpose((kv[:, HEAD_DIM:] + vb_ref[...]).astype(BF16))

    def moved(way, turn, sub, kind, s, hops):
        at = slot(pos - hops if way == 0 else pos + hops)
        first, count = (way ^ turn) * part_rows, part_rows // SUBS
        if kind:
            part = vbuf.at[at, way ^ turn, pl.ds(sub * (HEAD_DIM // SUBS), HEAD_DIM // SUBS)]
        else:
            part = kbuf.at[at, pl.ds(first + sub * count, count)]
        unit = (((s - 1) * 2 + turn) * 2 + way) * 2 * SUBS + sub * 2 + kind
        return pltpu.make_async_remote_copy(
            src_ref=part,
            dst_ref=part,
            send_sem=ring_send.at[kind],
            recv_sem=ring_recv.at[unit],
            device_id={"seq": ends[way]},
            device_id_type=MESH,
        )

    def send(way, turn, sub, kind, s):
        return moved(way, turn, sub, kind, s, s - 1)

    def arrival(way, turn, sub, kind, s):
        return moved(way, turn, sub, kind, s, s)

    def send_own(way, turn):
        for kind in (0, 1):
            for sub in range(SUBS):
                send(way, turn, sub, kind, 1).start()

    def forward(s, turn, go_on=True):
        for kind in (0, 1):
            for sub in range(SUBS):
                for way in (0, 1):
                    arrival(way, turn, sub, kind, s).wait_recv()
                    if go_on:
                        send(way, turn, sub, kind, s + 1).start()

    norm_half(0)
    tok_loads[1].wait()
    norm_half(1)
    for small in smalls:
        small.wait()
    limit = length_ref[0]
    for flat, row in ((kb_1d, kb_ref), (vb_1d, vb_ref), (qb_1d, qb_ref), (fgain_1d, fgain_ref)):
        spread(flat, row)
    lane = lax.broadcasted_iota(jnp.int32, (1, HEAD_DIM), 1)
    sign = jnp.where(lane < HEAD_DIM // 2, -1.0, 1.0)
    co, so = far[0, :1], far[1, :1]
    cos[...] = near[0] * co - near[1] * so
    sin[...] = (near[1] * co + near[0] * so) * sign
    for load in kv_loads:
        load.wait()
    project(0)
    pl.semaphore_wait(barrier, n_head + 1)

    @pl.when(mc == 0)
    def _():
        send_own(0, 0)

    project(1)

    @pl.when(mc == 0)
    def _():
        send_own(1, 0)
        send_own(0, 1)
        send_own(1, 1)

    def put_query(h, u):
        u = rope(u + qb_ref[:, h * HEAD_DIM : (h + 1) * HEAD_DIM]) * HEAD_DIM ** (-0.5)
        qt[:, h * rows : (h + 1) * rows] = jnp.transpose(u.astype(BF16))

    def queries(first):
        last = min(first + 4, heads)
        u = dot(normed[...], wq[:, first * HEAD_DIM : last * HEAD_DIM])
        for h in range(first, last):
            put_query(h, u[:, (h - first) * HEAD_DIM : (h - first + 1) * HEAD_DIM])

    def attend(blocks, poll=None, last=False, group=1):
        row_at = lax.broadcasted_iota(jnp.int32, (part_rows, 1), 0)
        live = [
            jnp.concatenate([b * rows + h * part_rows + row_at for b, h in block], axis=0) < limit
            for block in blocks
        ]

        def keys(block):
            parts = [kbuf[b, h * part_rows : (h + 1) * part_rows] for b, h in block]
            return jnp.concatenate(parts, axis=0)

        def values(block):
            return jnp.concatenate([vbuf[b, h] for b, h in block], axis=1)

        def span(h):
            return slice(h * rows, min(h + group, heads) * rows)

        def scores(h):
            return [
                jnp.where(ok, dot(keys(block), qt[:, span(h)]), LOW)
                for block, ok in zip(blocks, live)
            ]

        def weigh(h, many):
            old = m_ref[:, span(h)][:1]
            top = functools.reduce(
                jnp.maximum, [jnp.max(s, axis=0, keepdims=True) for s in many], old
            )
            m_ref[:, span(h)] = jnp.broadcast_to(top, (8, top.shape[1]))
            return h, jnp.exp(old - top), [jnp.exp(s - top).astype(BF16) for s in many]

        def mix(h, alpha, weights):
            new = None
            for block, p in zip(blocks, weights):
                more = dot(jnp.concatenate([values(block), ones], axis=0), p)
                new = more if new is None else new + more
            new = acc_ref[:, span(h)] * alpha + new
            if last:
                done = (new[:HEAD_DIM] / new[HEAD_DIM : HEAD_DIM + 1]).astype(BF16)
                for g in range(done.shape[1] // rows):
                    at = slice((h + g) * HEAD_DIM, (h + g + 1) * HEAD_DIM)
                    att[:, at] = jnp.transpose(done[:, g * rows : (g + 1) * rows])
            else:
                acc_ref[:, span(h)] = new

        ready, held = scores(0), None
        for h in range(0, heads, group):
            after = scores(h + group) if h + group < heads else None
            weighed = weigh(h, ready)
            if held is not None:
                mix(*held)
            held, ready = weighed, after
            if poll and h == heads // 2:
                poll()
        mix(*held)

    def whole(at):
        return ((at, 0), (at, 1))

    def pair(s):
        return [whole(slot(pos - s)), whole(slot(pos + s))]

    def cross_half(s, turn):
        return [((slot(pos - s), turn), (slot(pos + s), 1 - turn))]

    q_load.wait()
    o_load.start()
    queries(0)

    @pl.when(mc == 1)
    def _():
        for turn in (0, 1):
            for way in (0, 1):
                send_own(way, turn)

    for first in range(4, heads, 4):
        queries(first)
    forward(1, 0)
    attend([whole(ms)], group=GROUP)
    forward(1, 1)

    def ring_step(s, carry):
        attend(pair(s), lambda: forward(s + 1, 0))
        forward(s + 1, 1)
        return carry

    if half > 4:
        lax.fori_loop(1, half - 3, ring_step, 0)
    ring_step(half - 3, 0)
    attend(pair(half - 2), lambda: forward(half - 1, 0))
    forward(half - 1, 1, False)
    attend(pair(half - 1))
    forward(half, 0, False)
    attend(cross_half(half, 0), last=True, group=GROUP)
    o_load.wait()

    def far_y(d):
        return lax.rem(my + d, n_y)

    def partial(dest, at, wide):
        cols = pl.ds(pl.multiple_of(dest * share + at, HEAD_DIM), wide)
        return dot(att[...], wo[:, cols])

    def place(i):
        at, wide = chunks[i]
        return slice(at, at + wide)

    def pair_copy(i, d):
        return pltpu.make_async_remote_copy(
            src_ref=psend.at[d, :, place(i)],
            dst_ref=precv.at[d, :, place(i)],
            send_sem=pair_send.at[0],
            recv_sem=pair_recv.at[i, d],
            device_id=partner,
            device_id_type=MESH,
        )

    def cross_copy(i, d):
        return pltpu.make_async_remote_copy(
            src_ref=ysend.at[d - 1, :, place(i)],
            dst_ref=yrecv.at[d - 1, :, place(i)],
            send_sem=cross_send.at[0],
            recv_sem=cross_recv.at[i, d - 1],
            device_id={"head": 2 * far_y(d) + mc},
            device_id_type=MESH,
        )

    def part_sums(i, d):
        at, wide = chunks[i]
        psend[d, :, place(i)] = partial(2 * far_y(d) + 1 - mc, at, wide).astype(BF16)
        pair_copy(i, d).start()
        pown[d, :, place(i)] = partial(2 * far_y(d) + mc, at, wide)

    def across(i):
        for d in range(1, n_y):
            pair_copy(i, d).wait_recv()
            total = pown[d, :, place(i)] + precv[d, :, place(i)].astype(F32)
            ysend[d - 1, :, place(i)] = total.astype(BF16)
            cross_copy(i, d).start()

    @pl.when(mc == 0)
    def _():
        for i in range(len(chunks)):
            for d in range(1, n_y):
                part_sums(i, d)
            across(i)

    @pl.when(mc == 1)
    def _():
        for i in range(len(chunks)):
            for d in range(1, n_y):
                part_sums(i, d)
        for i in range(len(chunks)):
            across(i)

    for i in range(len(chunks)):
        part_sums(i, 0)

    squares = None
    for i, (at, wide) in enumerate(chunks):
        mine = pl.ds(pl.multiple_of(mh * share + at, HEAD_DIM), wide)
        pair_copy(i, 0).wait_recv()
        base = tok[:, mine].astype(F32) + (pown[0, :, place(i)] + precv[0, :, place(i)].astype(F32))
        for d in range(1, n_y):
            cross_copy(i, d).wait_recv()
            base = base + yrecv[d - 1, :, place(i)].astype(F32)
        hid[:, at : at + wide] = base
        hid_bf[:, at : at + wide] = base.astype(BF16)
        for g in range(0, wide, HEAD_DIM):
            piece = base[:, g : g + HEAD_DIM]
            squares = piece * piece if squares is None else squares + piece * piece

    def exchange(buf, axis, me, n, sems):
        def copy(d, slot_at):
            return pltpu.make_async_remote_copy(
                src_ref=buf.at[slot_at],
                dst_ref=buf.at[slot_at],
                send_sem=sems.at[0],
                recv_sem=sems.at[1],
                device_id={axis: lax.rem(me + d, n)},
                device_id_type=MESH,
            )

        for d in range(n - 1, 0, -1):
            copy(d, me).start()
        part = buf.at[pl.ds(0, n - 1)]
        pltpu.make_async_remote_copy(
            src_ref=part,
            dst_ref=part,
            send_sem=sems.at[0],
            recv_sem=sems.at[1],
            device_id=partner,
            device_id_type=MESH,
        ).wait_recv()

    def head_sum(buf, sems, value):
        buf[mh] = jnp.broadcast_to(value, buf.shape[1:])
        exchange(buf, "head", mh, n_head, sems)
        return functools.reduce(lambda a, b: a + b, [buf[d][:1] for d in range(n_head)])

    square_row = jnp.sum(jnp.transpose(squares), axis=0, keepdims=True)
    power = head_sum(sqbuf, sq_sem, square_row)
    where = ms * rows + lax.broadcasted_iota(jnp.int32, (1, rows), 1)
    scale = jnp.where(where < limit, lax.rsqrt(power / width + EPS), 0.0)
    scale = jnp.transpose(jnp.broadcast_to(scale, (HEAD_DIM, rows)))

    groups = pbuf.shape[1]
    sums = []
    for g in range(0, share, HEAD_DIM):
        at = slice(g, g + HEAD_DIM)
        sums.append(jnp.sum(hid[:, at] * scale, axis=0, keepdims=True) * fgain_ref[:, at])
    sums += [jnp.zeros((1, HEAD_DIM), F32)] * (groups - len(sums))
    pbuf[ms] = jnp.concatenate(sums, axis=0)

    exchange(pbuf, "seq", ms, n_seq, pool_sem)
    mean = functools.reduce(lambda a, b: a + b, [pbuf[d] for d in range(n_seq)])
    mean = mean / limit.astype(F32)
    total = head_sum(wbuf, pow_sem, jnp.sum(mean * mean, axis=0, keepdims=True))
    pooled = mean * lax.rsqrt(jnp.sum(total, axis=1, keepdims=True) / width + EPS)
    for g in range(share // HEAD_DIM):
        emb_ref[g * HEAD_DIM : (g + 1) * HEAD_DIM] = pooled[g : g + 1].reshape(HEAD_DIM)

    def all_sent(ref, sems, n):
        part = ref.at[pl.ds(0, n)]
        pltpu.make_async_remote_copy(
            src_ref=part,
            dst_ref=part,
            send_sem=sems.at[0],
            recv_sem=sems.at[0],
            device_id=partner,
            device_id_type=MESH,
        ).wait_send()

    all_sent(kbuf, ring_send.at[pl.ds(0, 1)], n_seq - 1)
    all_sent(vbuf, ring_send.at[pl.ds(1, 1)], n_seq - 1)
    all_sent(psend, pair_send, n_y)
    all_sent(ysend, cross_send, n_y - 1)
    all_sent(sqbuf, sq_sem, n_head - 1)
    all_sent(pbuf, pool_sem, n_seq - 1)
    all_sent(wbuf, pow_sem, n_head - 1)


def write_out(hidden_ref, emb_ref, hidden_hbm, emb_hbm, sems):
    copies = [
        pltpu.make_async_copy(hidden_ref, hidden_hbm, sems.at[0]),
        pltpu.make_async_copy(emb_ref, emb_hbm, sems.at[1]),
    ]
    for copy in copies:
        copy.start()
    for copy in copies:
        copy.wait()


def body(
    n_seq,
    n_head,
    tokens,
    length,
    in_gain,
    q_weight,
    q_bias,
    k_weight,
    k_bias,
    v_weight,
    v_bias,
    o_weight,
    final_gain,
):
    rows, width = tokens.shape
    share = width // n_head
    heads = q_weight.shape[1] // HEAD_DIM
    half = n_seq // 2
    n_y = n_head // 2
    inverse = ROPE_BASE ** (-(np.arange(HEAD_DIM // 2) * 2.0) / HEAD_DIM)
    inverse = np.concatenate([inverse, inverse])[None, :]
    near = np.arange(rows)[:, None] * inverse
    near = np.stack([np.cos(near), np.sin(near)]).astype(np.float32)
    far = (np.arange(n_seq) * rows)[:, None] * inverse
    far = np.stack([np.cos(far), np.sin(far)], axis=1).astype(np.float32)
    far = np.repeat(far[:, :, None, :], 8, axis=2)

    chunks = widths(share)
    groups = -(-share // (8 * HEAD_DIM)) * 8
    dma = pltpu.SemaphoreType.DMA
    hbm = pl.BlockSpec(memory_space=pltpu.HBM)
    vmem = pl.BlockSpec(memory_space=pltpu.VMEM)
    shapes = (
        jax.ShapeDtypeStruct((rows, share), BF16),
        jax.ShapeDtypeStruct((share,), F32),
    )
    operands = (
        length,
        tokens,
        in_gain,
        q_weight,
        q_bias,
        k_weight,
        k_bias,
        v_weight,
        v_bias,
        o_weight,
        final_gain,
        jnp.asarray(near),
        jnp.asarray(far),
    )
    hidden, embedding = pl.pallas_call(
        functools.partial(kernel, n_seq, n_head),
        out_shape=shapes,
        in_specs=[hbm] * 13,
        out_specs=(vmem, vmem),
        scratch_shapes=[
            pltpu.SMEM((1,), jnp.int32),
            pltpu.VMEM((width,), F32),
            pltpu.VMEM((heads * HEAD_DIM,), F32),
            pltpu.VMEM((HEAD_DIM,), F32),
            pltpu.VMEM((HEAD_DIM,), F32),
            pltpu.VMEM((share,), F32),
            pltpu.VMEM(near.shape, F32),
            pltpu.VMEM(far.shape[1:], F32),
            pltpu.VMEM((1, width), F32),
            pltpu.VMEM((1, heads * HEAD_DIM), F32),
            pltpu.VMEM((1, HEAD_DIM), F32),
            pltpu.VMEM((1, HEAD_DIM), F32),
            pltpu.VMEM((1, share), F32),
            pltpu.VMEM((rows, width), BF16),
            pltpu.VMEM((rows, width), BF16),
            pltpu.VMEM((width, 2 * HEAD_DIM), BF16),
            pltpu.VMEM(q_weight.shape, BF16),
            pltpu.VMEM(o_weight.shape, BF16),
            pltpu.VMEM((rows, HEAD_DIM), F32),
            pltpu.VMEM((rows, HEAD_DIM), F32),
            pltpu.VMEM((HEAD_DIM, heads * rows), BF16),
            pltpu.VMEM((n_seq, rows, HEAD_DIM), BF16),
            pltpu.VMEM((n_seq, 2, HEAD_DIM, rows // 2), BF16),
            pltpu.VMEM((8, heads * rows), F32),
            pltpu.VMEM((HEAD_DIM + 16, heads * rows), F32),
            pltpu.VMEM((rows, heads * HEAD_DIM), BF16),
            pltpu.VMEM((rows, share), F32),
            pltpu.VMEM((n_y, rows, share), BF16),
            pltpu.VMEM((n_y, rows, share), BF16),
            pltpu.VMEM((n_y, rows, share), F32),
            pltpu.VMEM((n_y - 1, rows, share), BF16),
            pltpu.VMEM((n_y - 1, rows, share), BF16),
            pltpu.VMEM((n_head, 8, rows), F32),
            pltpu.VMEM((n_seq, groups, HEAD_DIM), F32),
            pltpu.VMEM((n_head, 8, HEAD_DIM), F32),
            dma((14,)),
            dma((2,)),
            dma((SUBS * (8 * half - 4),)),
            dma((1,)),
            dma((len(chunks), n_y)),
            dma((1,)),
            dma((len(chunks), n_y - 1)),
            dma((2,)),
            dma((2,)),
            dma((2,)),
        ],
        compiler_params=pltpu.CompilerParams(
            collective_id=0, has_side_effects=True, vmem_limit_bytes=48 * 1024 * 1024
        ),
    )(operands[0], *[pltpu.with_memory_space_constraint(x, pltpu.HBM) for x in operands[1:]])
    return pl.pallas_call(
        write_out,
        out_shape=shapes,
        in_specs=[vmem, vmem],
        out_specs=(hbm, hbm),
        scratch_shapes=[dma((2,))],
        compiler_params=pltpu.CompilerParams(vmem_limit_bytes=2 * 1024 * 1024),
    )(hidden, embedding)


def solution(mesh):
    in_specs = (
        P("seq", None),
        P(),
        P(),
        P(None, "head"),
        P("head"),
        P(None, "head"),
        P("head"),
        P(None, "head"),
        P("head"),
        P("head", None),
        P("head"),
    )
    out_specs = (P("seq", "head"), P("head"))
    step = functools.partial(body, mesh.shape["seq"], mesh.shape["head"])
    return jax.shard_map(step, mesh=mesh, in_specs=in_specs, out_specs=out_specs, check_vma=False)
```

```python
import functools

import jax
import jax.numpy as jnp
import numpy as np
from jax import lax
from jax.experimental import pallas as pl
from jax.experimental.pallas import tpu as pltpu
from jax.sharding import PartitionSpec as P

HEAD_DIM = 128
ROPE_BASE = 1000000.0
EPS = 1e-06
MESH = pl.DeviceIdType.MESH
F32 = jnp.float32
BF16 = jnp.bfloat16
LOW = -1e30
SUBS = 1
GROUP = 4


def widths(share):
    out, at = [], 0
    while at < share:
        width = 128 if at == 0 or share - at <= 256 else 256
        out.append((at, width))
        at += width
    return out


def dot(a, b):
    return jnp.dot(a, b, preferred_element_type=F32)


def kernel(
    n_seq,
    n_head,
    length_hbm,
    tokens_hbm,
    gain_hbm,
    wq_hbm,
    qb_hbm,
    wk_hbm,
    kb_hbm,
    wv_hbm,
    vb_hbm,
    wo_hbm,
    fgain_hbm,
    near_hbm,
    far_hbm,
    hid_bf,
    emb_ref,
    length_ref,
    gain_1d,
    qb_1d,
    kb_1d,
    vb_1d,
    fgain_1d,
    near,
    far,
    gain_ref,
    qb_ref,
    kb_ref,
    vb_ref,
    fgain_ref,
    tok,
    normed,
    wkv,
    wq,
    wo,
    cos,
    sin,
    qt,
    kbuf,
    vbuf,
    m_ref,
    acc_ref,
    att,
    hid,
    psend,
    precv,
    pown,
    ysend,
    yrecv,
    sqbuf,
    pbuf,
    wbuf,
    shared,
    other,
    local_sem,
    ring_send,
    ring_recv,
    pair_send,
    pair_recv,
    cross_send,
    cross_recv,
    sq_sem,
    pool_sem,
    pow_sem,
    share_sem,
):
    rows, width = tok.shape
    share = hid.shape[1]
    heads = qt.shape[1] // rows
    part_rows = rows // 2
    half = n_seq // 2
    n_y = n_head // 2
    chunks = widths(share)
    ms = lax.axis_index("seq")
    mh = lax.axis_index("head")

    def band(h):
        return pl.ds(h * part_rows, part_rows)

    def quarter(i):
        return pl.ds(i * (rows // 4), rows // 4)

    tok_loads = [
        pltpu.make_async_copy(tokens_hbm.at[quarter(i)], tok.at[quarter(i)], local_sem.at[i])
        for i in range(4)
    ]
    kv_loads = [
        pltpu.make_async_copy(wk_hbm, wkv.at[:, :HEAD_DIM], local_sem.at[4]),
        pltpu.make_async_copy(wv_hbm, wkv.at[:, HEAD_DIM:], local_sem.at[5]),
    ]
    q_load = pltpu.make_async_copy(wq_hbm, wq, local_sem.at[6])
    o_load = pltpu.make_async_copy(wo_hbm, wo, local_sem.at[7])
    gain_load = pltpu.make_async_copy(gain_hbm, gain_1d, local_sem.at[8])
    smalls = [
        pltpu.make_async_copy(near_hbm, near, local_sem.at[9]),
        pltpu.make_async_copy(far_hbm.at[ms], far, local_sem.at[10]),
        pltpu.make_async_copy(kb_hbm, kb_1d, local_sem.at[11]),
        pltpu.make_async_copy(vb_hbm, vb_1d, local_sem.at[12]),
        pltpu.make_async_copy(qb_hbm, qb_1d, local_sem.at[13]),
        pltpu.make_async_copy(fgain_hbm, fgain_1d, local_sem.at[14]),
        pltpu.make_async_copy(length_hbm, length_ref, local_sem.at[15]),
    ]
    for load in [tok_loads[0], gain_load, *tok_loads[1:], *kv_loads, *smalls, q_load]:
        load.start()

    q2 = lax.div(ms, 2)
    pos = q2 + (ms - 2 * q2) * (n_seq - 1 - 2 * q2)

    def slot(p):
        p = lax.rem(p + 2 * n_seq, n_seq)
        back = lax.div(p, half)
        return (1 - back) * 2 * p + back * (2 * (n_seq - 1 - p) + 1)

    ends = (slot(pos + 1), slot(pos - 1))
    my = lax.div(mh, 2)
    mc = mh - 2 * my
    partner = {"head": 2 * my + 1 - mc}
    barrier = pltpu.get_barrier_semaphore()
    for end in ends:
        pl.semaphore_signal(barrier, inc=1, device_id={"seq": end}, device_id_type=MESH)
    for d in range(1, n_head):
        pl.semaphore_signal(
            barrier, inc=1, device_id={"head": lax.rem(mh + d, n_head)}, device_id_type=MESH
        )

    def spread(flat, row):
        for g in range(0, row.shape[1], HEAD_DIM):
            row[:, g : g + HEAD_DIM] = flat[g : g + HEAD_DIM].reshape(1, HEAD_DIM)

    m_ref[...] = jnp.full(m_ref.shape, LOW, F32)
    acc_ref[...] = jnp.zeros(acc_ref.shape, F32)
    ones = lax.broadcasted_iota(jnp.int32, (16, rows), 0)
    ones = jnp.where(ones == 0, 1.0, 0.0).astype(BF16)

    gain_load.wait()
    spread(gain_1d, gain_ref)
    block = 16

    def norm_quarter(q):
        for k in range(rows // 4 // block):
            at = pl.ds(q * (rows // 4) + k * block, block)
            x = tok[at, :].astype(F32)
            mean = jnp.sum(x * x, axis=1, keepdims=True) / width
            normed[at, :] = (x * lax.rsqrt(mean + EPS) * gain_ref[...]).astype(BF16)

    def rope(u, h=None):
        at = slice(None) if h is None else band(h)
        return u * cos[at, :] + pltpu.roll(u, HEAD_DIM // 2, 1) * sin[at, :]

    def project(h):
        kv = dot(normed[band(h), :], wkv[...])
        kbuf[ms, band(h)] = rope(kv[:, :HEAD_DIM] + kb_ref[...], h).astype(BF16)
        vbuf[ms, h] = jnp.transpose((kv[:, HEAD_DIM:] + vb_ref[...]).astype(BF16))

    def moved(way, turn, sub, kind, s, hops):
        at = slot(pos - hops if way == 0 else pos + hops)
        first, count = (way ^ turn) * part_rows, part_rows // SUBS
        if kind:
            part = vbuf.at[at, way ^ turn, pl.ds(sub * (HEAD_DIM // SUBS), HEAD_DIM // SUBS)]
        else:
            part = kbuf.at[at, pl.ds(first + sub * count, count)]
        unit = (((s - 1) * 2 + turn) * 2 + way) * 2 * SUBS + sub * 2 + kind
        return pltpu.make_async_remote_copy(
            src_ref=part,
            dst_ref=part,
            send_sem=ring_send.at[kind],
            recv_sem=ring_recv.at[unit],
            device_id={"seq": ends[way]},
            device_id_type=MESH,
        )

    def send(way, turn, sub, kind, s):
        return moved(way, turn, sub, kind, s, s - 1)

    def arrival(way, turn, sub, kind, s):
        return moved(way, turn, sub, kind, s, s)

    def send_own(way, turn):
        for kind in (0, 1):
            for sub in range(SUBS):
                send(way, turn, sub, kind, 1).start()

    def arrive(s, turn, kind):
        for sub in range(SUBS):
            for way in (0, 1):
                arrival(way, turn, sub, kind, s).wait_recv()

    def forward(s, turn):
        for kind in (0, 1):
            for sub in range(SUBS):
                for way in (0, 1):
                    arrival(way, turn, sub, kind, s).wait_recv()
                    send(way, turn, sub, kind, s + 1).start()

    for q in range(4):
        tok_loads[q].wait()
        norm_quarter(q)
    for small in smalls:
        small.wait()
    limit = length_ref[0]
    for flat, row in ((kb_1d, kb_ref), (vb_1d, vb_ref), (qb_1d, qb_ref), (fgain_1d, fgain_ref)):
        spread(flat, row)
    lane = lax.broadcasted_iota(jnp.int32, (1, HEAD_DIM), 1)
    sign = jnp.where(lane < HEAD_DIM // 2, -1.0, 1.0)
    co, so = far[0, :1], far[1, :1]
    cos[...] = near[0] * co - near[1] * so
    sin[...] = (near[1] * co + near[0] * so) * sign
    for load in kv_loads:
        load.wait()
    project(0)
    pl.semaphore_wait(barrier, n_head + 1)

    @pl.when(mc == 0)
    def _():
        send_own(0, 0)

    project(1)

    @pl.when(mc == 0)
    def _():
        send_own(1, 0)
        send_own(0, 1)
        send_own(1, 1)

    def put_query(h, u):
        u = rope(u + qb_ref[:, h * HEAD_DIM : (h + 1) * HEAD_DIM]) * HEAD_DIM ** (-0.5)
        qt[:, h * rows : (h + 1) * rows] = jnp.transpose(u.astype(BF16))

    def queries(first):
        last = min(first + 4, heads)
        u = dot(normed[...], wq[:, first * HEAD_DIM : last * HEAD_DIM])
        for h in range(first, last):
            put_query(h, u[:, (h - first) * HEAD_DIM : (h - first + 1) * HEAD_DIM])

    def attend(blocks, poll=None, last=False, group=1, values_in=None):
        row_at = lax.broadcasted_iota(jnp.int32, (part_rows, 1), 0)
        live = [
            jnp.concatenate([b * rows + h * part_rows + row_at for b, h in block], axis=0) < limit
            for block in blocks
        ]

        def keys(block):
            parts = [kbuf[b, h * part_rows : (h + 1) * part_rows] for b, h in block]
            return jnp.concatenate(parts, axis=0)

        def values(block):
            return jnp.concatenate([vbuf[b, h] for b, h in block], axis=1)

        def span(h):
            return slice(h * rows, min(h + group, heads) * rows)

        def scores(h):
            return [
                jnp.where(ok, dot(keys(block), qt[:, span(h)]), LOW)
                for block, ok in zip(blocks, live)
            ]

        def weigh(h, many):
            old = m_ref[:, span(h)][:1]
            top = functools.reduce(
                jnp.maximum, [jnp.max(s, axis=0, keepdims=True) for s in many], old
            )
            m_ref[:, span(h)] = jnp.broadcast_to(top, (8, top.shape[1]))
            return h, jnp.exp(old - top), [jnp.exp(s - top).astype(BF16) for s in many]

        def mix(h, alpha, weights):
            new = None
            for block, p in zip(blocks, weights):
                more = dot(jnp.concatenate([values(block), ones], axis=0), p)
                new = more if new is None else new + more
            new = acc_ref[:, span(h)] * alpha + new
            if last:
                done = (new[:HEAD_DIM] / new[HEAD_DIM : HEAD_DIM + 1]).astype(BF16)
                for g in range(done.shape[1] // rows):
                    at = slice((h + g) * HEAD_DIM, (h + g + 1) * HEAD_DIM)
                    att[:, at] = jnp.transpose(done[:, g * rows : (g + 1) * rows])
            else:
                acc_ref[:, span(h)] = new

        ready, held = scores(0), None
        for h in range(0, heads, group):
            after = scores(h + group) if h + group < heads else None
            weighed = weigh(h, ready)
            if h == 0 and values_in:
                values_in()
            if held is not None:
                mix(*held)
            held, ready = weighed, after
            if poll and h == heads // 2:
                poll()
        mix(*held)

    def whole(at):
        return ((at, 0), (at, 1))

    def pair(s):
        return [whole(slot(pos - s)), whole(slot(pos + s))]

    def cross_half(s, turn):
        return [((slot(pos - s), turn), (slot(pos + s), 1 - turn))]

    q_load.wait()
    o_load.start()
    queries(0)

    @pl.when(mc == 1)
    def _():
        for turn in (0, 1):
            for way in (0, 1):
                send_own(way, turn)

    for first in range(4, heads, 4):
        queries(first)
    forward(1, 0)
    attend([whole(ms)], group=GROUP)
    forward(1, 1)

    def ring_step(s, carry):
        attend(pair(s), lambda: forward(s + 1, 0))
        forward(s + 1, 1)
        return carry

    if half > 4:
        lax.fori_loop(1, half - 3, ring_step, 0)
    ring_step(half - 3, 0)
    attend(pair(half - 2), lambda: forward(half - 1, 0))
    arrive(half - 1, 1, 0)
    attend(pair(half - 1), values_in=lambda: arrive(half - 1, 1, 1))
    arrive(half, 0, 0)
    attend(
        cross_half(half, 0), last=True, group=GROUP, values_in=lambda: arrive(half, 0, 1)
    )
    o_load.wait()

    def far_y(d):
        return lax.rem(my + d, n_y)

    def partial(dest, at, wide):
        cols = pl.ds(pl.multiple_of(dest * share + at, HEAD_DIM), wide)
        return dot(att[...], wo[:, cols])

    def place(i):
        at, wide = chunks[i]
        return slice(at, at + wide)

    def pair_copy(i, d):
        return pltpu.make_async_remote_copy(
            src_ref=psend.at[d, :, place(i)],
            dst_ref=precv.at[d, :, place(i)],
            send_sem=pair_send.at[0],
            recv_sem=pair_recv.at[i, d],
            device_id=partner,
            device_id_type=MESH,
        )

    def cross_copy(i, d):
        return pltpu.make_async_remote_copy(
            src_ref=ysend.at[d - 1, :, place(i)],
            dst_ref=yrecv.at[d - 1, :, place(i)],
            send_sem=cross_send.at[0],
            recv_sem=cross_recv.at[i, d - 1],
            device_id={"head": 2 * far_y(d) + mc},
            device_id_type=MESH,
        )

    def part_sums(i, d):
        at, wide = chunks[i]
        psend[d, :, place(i)] = partial(2 * far_y(d) + 1 - mc, at, wide).astype(BF16)
        pair_copy(i, d).start()
        pown[d, :, place(i)] = partial(2 * far_y(d) + mc, at, wide)

    def across(i):
        for d in range(1, n_y):
            pair_copy(i, d).wait_recv()
            total = pown[d, :, place(i)] + precv[d, :, place(i)].astype(F32)
            ysend[d - 1, :, place(i)] = total.astype(BF16)
            cross_copy(i, d).start()

    @pl.when(mc == 0)
    def _():
        for i in range(len(chunks)):
            for d in range(1, n_y):
                part_sums(i, d)
            across(i)

    @pl.when(mc == 1)
    def _():
        for i in range(len(chunks)):
            for d in range(1, n_y):
                part_sums(i, d)
        for i in range(len(chunks)):
            across(i)

    for i in range(len(chunks)):
        part_sums(i, 0)

    squares = None
    for i, (at, wide) in enumerate(chunks):
        mine = pl.ds(pl.multiple_of(mh * share + at, HEAD_DIM), wide)
        pair_copy(i, 0).wait_recv()
        base = tok[:, mine].astype(F32) + (pown[0, :, place(i)] + precv[0, :, place(i)].astype(F32))
        for d in range(1, n_y):
            cross_copy(i, d).wait_recv()
            base = base + yrecv[d - 1, :, place(i)].astype(F32)
        hid[:, at : at + wide] = base
        hid_bf[:, at : at + wide] = base.astype(BF16)
        for g in range(0, wide, HEAD_DIM):
            piece = base[:, g : g + HEAD_DIM]
            squares = piece * piece if squares is None else squares + piece * piece

    def exchange(buf, axis, me, n, sems):
        def copy(d, slot_at):
            return pltpu.make_async_remote_copy(
                src_ref=buf.at[slot_at],
                dst_ref=buf.at[slot_at],
                send_sem=sems.at[0],
                recv_sem=sems.at[1],
                device_id={axis: lax.rem(me + d, n)},
                device_id_type=MESH,
            )

        for d in range(n - 1, 0, -1):
            copy(d, me).start()
        part = buf.at[pl.ds(0, n - 1)]
        pltpu.make_async_remote_copy(
            src_ref=part,
            dst_ref=part,
            send_sem=sems.at[0],
            recv_sem=sems.at[1],
            device_id=partner,
            device_id_type=MESH,
        ).wait_recv()

    def head_sum(buf, sems, value):
        buf[mh] = jnp.broadcast_to(value, buf.shape[1:])
        exchange(buf, "head", mh, n_head, sems)
        return functools.reduce(lambda a, b: a + b, [buf[d][:1] for d in range(n_head)])

    square_row = jnp.sum(jnp.transpose(squares), axis=0, keepdims=True)
    power = head_sum(sqbuf, sq_sem, square_row)
    where = ms * rows + lax.broadcasted_iota(jnp.int32, (1, rows), 1)
    scale = jnp.where(where < limit, lax.rsqrt(power / width + EPS), 0.0)
    scale = jnp.transpose(jnp.broadcast_to(scale, (HEAD_DIM, rows)))

    groups = pbuf.shape[1]
    sums = []
    for g in range(0, share, HEAD_DIM):
        at = slice(g, g + HEAD_DIM)
        sums.append(jnp.sum(hid[:, at] * scale, axis=0, keepdims=True) * fgain_ref[:, at])
    sums += [jnp.zeros((1, HEAD_DIM), F32)] * (groups - len(sums))
    pbuf[ms] = jnp.concatenate(sums, axis=0)

    shared[...] = pbuf[ms].astype(BF16)

    def share_copy(d):
        return pltpu.make_async_remote_copy(
            src_ref=shared,
            dst_ref=other.at[ms],
            send_sem=share_sem.at[0],
            recv_sem=share_sem.at[1],
            device_id={"seq": lax.rem(ms + d, n_seq), **partner},
            device_id_type=MESH,
        )

    for d in range(n_seq - 1, -1, -1):
        share_copy(d).start()
    exchange(pbuf, "seq", ms, n_seq, pool_sem)
    every_share = pltpu.make_async_remote_copy(
        src_ref=other,
        dst_ref=other,
        send_sem=share_sem.at[0],
        recv_sem=share_sem.at[1],
        device_id=partner,
        device_id_type=MESH,
    )
    every_share.wait_recv()
    mean = functools.reduce(lambda a, b: a + b, [pbuf[d] for d in range(n_seq)])
    mean = mean / limit.astype(F32)
    near_mean = functools.reduce(
        lambda a, b: a + b, [other[d].astype(F32) for d in range(n_seq)]
    )
    near_mean = near_mean / limit.astype(F32)
    power = jnp.sum(mean * mean + near_mean * near_mean, axis=0, keepdims=True)
    wbuf[my] = jnp.broadcast_to(power, wbuf.shape[1:])

    @pl.when(mc == 1)
    def _():
        for d in range(1, n_y):
            for c in (0, 1):
                pltpu.make_async_remote_copy(
                    src_ref=wbuf.at[my],
                    dst_ref=wbuf.at[my],
                    send_sem=pow_sem.at[0],
                    recv_sem=pow_sem.at[1],
                    device_id={"head": 2 * far_y(d) + c},
                    device_id_type=MESH,
                ).start()

    part = wbuf.at[pl.ds(0, n_y - 1)]
    pltpu.make_async_remote_copy(
        src_ref=part,
        dst_ref=part,
        send_sem=pow_sem.at[0],
        recv_sem=pow_sem.at[1],
        device_id=partner,
        device_id_type=MESH,
    ).wait_recv()
    total = functools.reduce(lambda a, b: a + b, [wbuf[y][:1] for y in range(n_y)])
    pooled = mean * lax.rsqrt(jnp.sum(total, axis=1, keepdims=True) / width + EPS)
    for g in range(share // HEAD_DIM):
        emb_ref[g * HEAD_DIM : (g + 1) * HEAD_DIM] = pooled[g : g + 1].reshape(HEAD_DIM)

    def all_sent(ref, sems, n):
        part = ref.at[pl.ds(0, n)]
        pltpu.make_async_remote_copy(
            src_ref=part,
            dst_ref=part,
            send_sem=sems.at[0],
            recv_sem=sems.at[0],
            device_id=partner,
            device_id_type=MESH,
        ).wait_send()

    all_sent(kbuf, ring_send.at[pl.ds(0, 1)], n_seq - 1)
    all_sent(vbuf, ring_send.at[pl.ds(1, 1)], n_seq - 1)
    all_sent(psend, pair_send, n_y)
    all_sent(ysend, cross_send, n_y - 1)
    all_sent(sqbuf, sq_sem, n_head - 1)
    all_sent(pbuf, pool_sem, n_seq - 1)
    every_share.wait_send()

    @pl.when(mc == 1)
    def _():
        all_sent(wbuf, pow_sem, 2 * (n_y - 1))


def write_out(hidden_ref, emb_ref, hidden_hbm, emb_hbm, sems):
    copies = [
        pltpu.make_async_copy(hidden_ref, hidden_hbm, sems.at[0]),
        pltpu.make_async_copy(emb_ref, emb_hbm, sems.at[1]),
    ]
    for copy in copies:
        copy.start()
    for copy in copies:
        copy.wait()


def body(
    n_seq,
    n_head,
    tokens,
    length,
    in_gain,
    q_weight,
    q_bias,
    k_weight,
    k_bias,
    v_weight,
    v_bias,
    o_weight,
    final_gain,
):
    rows, width = tokens.shape
    share = width // n_head
    heads = q_weight.shape[1] // HEAD_DIM
    half = n_seq // 2
    n_y = n_head // 2
    inverse = ROPE_BASE ** (-(np.arange(HEAD_DIM // 2) * 2.0) / HEAD_DIM)
    inverse = np.concatenate([inverse, inverse])[None, :]
    near = np.arange(rows)[:, None] * inverse
    near = np.stack([np.cos(near), np.sin(near)]).astype(np.float32)
    far = (np.arange(n_seq) * rows)[:, None] * inverse
    far = np.stack([np.cos(far), np.sin(far)], axis=1).astype(np.float32)
    far = np.repeat(far[:, :, None, :], 8, axis=2)

    chunks = widths(share)
    groups = -(-share // (8 * HEAD_DIM)) * 8
    dma = pltpu.SemaphoreType.DMA
    hbm = pl.BlockSpec(memory_space=pltpu.HBM)
    vmem = pl.BlockSpec(memory_space=pltpu.VMEM)
    shapes = (
        jax.ShapeDtypeStruct((rows, share), BF16),
        jax.ShapeDtypeStruct((share,), F32),
    )
    operands = (
        length,
        tokens,
        in_gain,
        q_weight,
        q_bias,
        k_weight,
        k_bias,
        v_weight,
        v_bias,
        o_weight,
        final_gain,
        jnp.asarray(near),
        jnp.asarray(far),
    )
    hidden, embedding = pl.pallas_call(
        functools.partial(kernel, n_seq, n_head),
        out_shape=shapes,
        in_specs=[hbm] * 13,
        out_specs=(vmem, vmem),
        scratch_shapes=[
            pltpu.SMEM((1,), jnp.int32),
            pltpu.VMEM((width,), F32),
            pltpu.VMEM((heads * HEAD_DIM,), F32),
            pltpu.VMEM((HEAD_DIM,), F32),
            pltpu.VMEM((HEAD_DIM,), F32),
            pltpu.VMEM((share,), F32),
            pltpu.VMEM(near.shape, F32),
            pltpu.VMEM(far.shape[1:], F32),
            pltpu.VMEM((1, width), F32),
            pltpu.VMEM((1, heads * HEAD_DIM), F32),
            pltpu.VMEM((1, HEAD_DIM), F32),
            pltpu.VMEM((1, HEAD_DIM), F32),
            pltpu.VMEM((1, share), F32),
            pltpu.VMEM((rows, width), BF16),
            pltpu.VMEM((rows, width), BF16),
            pltpu.VMEM((width, 2 * HEAD_DIM), BF16),
            pltpu.VMEM(q_weight.shape, BF16),
            pltpu.VMEM(o_weight.shape, BF16),
            pltpu.VMEM((rows, HEAD_DIM), F32),
            pltpu.VMEM((rows, HEAD_DIM), F32),
            pltpu.VMEM((HEAD_DIM, heads * rows), BF16),
            pltpu.VMEM((n_seq, rows, HEAD_DIM), BF16),
            pltpu.VMEM((n_seq, 2, HEAD_DIM, rows // 2), BF16),
            pltpu.VMEM((8, heads * rows), F32),
            pltpu.VMEM((HEAD_DIM + 16, heads * rows), F32),
            pltpu.VMEM((rows, heads * HEAD_DIM), BF16),
            pltpu.VMEM((rows, share), F32),
            pltpu.VMEM((n_y, rows, share), BF16),
            pltpu.VMEM((n_y, rows, share), BF16),
            pltpu.VMEM((n_y, rows, share), F32),
            pltpu.VMEM((n_y - 1, rows, share), BF16),
            pltpu.VMEM((n_y - 1, rows, share), BF16),
            pltpu.VMEM((n_head, 8, rows), F32),
            pltpu.VMEM((n_seq, groups, HEAD_DIM), F32),
            pltpu.VMEM((n_head, 8, HEAD_DIM), F32),
            pltpu.VMEM((groups, HEAD_DIM), BF16),
            pltpu.VMEM((n_seq, groups, HEAD_DIM), BF16),
            dma((16,)),
            dma((2,)),
            dma((SUBS * (8 * half - 4),)),
            dma((1,)),
            dma((len(chunks), n_y)),
            dma((1,)),
            dma((len(chunks), n_y - 1)),
            dma((2,)),
            dma((2,)),
            dma((2,)),
            dma((2,)),
        ],
        compiler_params=pltpu.CompilerParams(
            collective_id=0, has_side_effects=True, vmem_limit_bytes=48 * 1024 * 1024
        ),
    )(operands[0], *[pltpu.with_memory_space_constraint(x, pltpu.HBM) for x in operands[1:]])
    return pl.pallas_call(
        write_out,
        out_shape=shapes,
        in_specs=[vmem, vmem],
        out_specs=(hbm, hbm),
        scratch_shapes=[dma((2,))],
        compiler_params=pltpu.CompilerParams(vmem_limit_bytes=2 * 1024 * 1024),
    )(hidden, embedding)


def solution(mesh):
    in_specs = (
        P("seq", None),
        P(),
        P(),
        P(None, "head"),
        P("head"),
        P(None, "head"),
        P("head"),
        P(None, "head"),
        P("head"),
        P("head", None),
        P("head"),
    )
    out_specs = (P("seq", "head"), P("head"))
    step = functools.partial(body, mesh.shape["seq"], mesh.shape["head"])
    return jax.shard_map(step, mesh=mesh, in_specs=in_specs, out_specs=out_specs, check_vma=False)
```

```python
import functools

import jax
import jax.numpy as jnp
import numpy as np
from jax import lax
from jax.experimental import pallas as pl
from jax.experimental.pallas import tpu as pltpu
from jax.sharding import PartitionSpec as P

HEAD_DIM = 128
ROPE_BASE = 1000000.0
EPS = 1e-06
MESH = pl.DeviceIdType.MESH
F32 = jnp.float32
BF16 = jnp.bfloat16
LOW = -1e30
SUBS = 1
GROUP = 4


def widths(share):
    out, at = [], 0
    while at < share:
        width = 128 if at == 0 or share - at <= 256 else 256
        out.append((at, width))
        at += width
    return out


def dot(a, b):
    return jnp.dot(a, b, preferred_element_type=F32)


def kernel(
    n_seq,
    n_head,
    length_hbm,
    tokens_hbm,
    gain_hbm,
    wq_hbm,
    qb_hbm,
    wk_hbm,
    kb_hbm,
    wv_hbm,
    vb_hbm,
    wo_hbm,
    fgain_hbm,
    near_hbm,
    far_hbm,
    hid_bf,
    emb_ref,
    length_ref,
    gain_1d,
    qb_1d,
    kb_1d,
    vb_1d,
    fgain_1d,
    near,
    far,
    gain_ref,
    qb_ref,
    kb_ref,
    vb_ref,
    fgain_ref,
    tok,
    normed,
    wkv,
    wq,
    wo,
    cos,
    sin,
    qt,
    kbuf,
    vbuf,
    m_ref,
    acc_ref,
    att,
    hid,
    psend,
    precv,
    pown,
    ysend,
    yrecv,
    sqbuf,
    pbuf,
    wbuf,
    shared,
    other,
    local_sem,
    ring_send,
    ring_recv,
    pair_send,
    pair_recv,
    cross_send,
    cross_recv,
    sq_sem,
    pool_sem,
    pow_sem,
    share_sem,
):
    rows, width = tok.shape
    share = hid.shape[1]
    heads = qt.shape[1] // rows
    part_rows = rows // 2
    half = n_seq // 2
    n_y = n_head // 2
    chunks = widths(share)
    ms = lax.axis_index("seq")
    mh = lax.axis_index("head")

    def band(h):
        return pl.ds(h * part_rows, part_rows)

    def quarter(i):
        return pl.ds(i * (rows // 4), rows // 4)

    tok_loads = [
        pltpu.make_async_copy(tokens_hbm.at[quarter(i)], tok.at[quarter(i)], local_sem.at[i])
        for i in range(4)
    ]
    kv_loads = [
        pltpu.make_async_copy(wk_hbm, wkv.at[:, :HEAD_DIM], local_sem.at[4]),
        pltpu.make_async_copy(wv_hbm, wkv.at[:, HEAD_DIM:], local_sem.at[5]),
    ]
    q_load = pltpu.make_async_copy(wq_hbm, wq, local_sem.at[6])
    o_load = pltpu.make_async_copy(wo_hbm, wo, local_sem.at[7])
    gain_load = pltpu.make_async_copy(gain_hbm, gain_1d, local_sem.at[8])
    smalls = [
        pltpu.make_async_copy(near_hbm, near, local_sem.at[9]),
        pltpu.make_async_copy(far_hbm.at[ms], far, local_sem.at[10]),
        pltpu.make_async_copy(kb_hbm, kb_1d, local_sem.at[11]),
        pltpu.make_async_copy(vb_hbm, vb_1d, local_sem.at[12]),
        pltpu.make_async_copy(qb_hbm, qb_1d, local_sem.at[13]),
        pltpu.make_async_copy(fgain_hbm, fgain_1d, local_sem.at[14]),
        pltpu.make_async_copy(length_hbm, length_ref, local_sem.at[15]),
    ]
    for load in [tok_loads[0], gain_load, *tok_loads[1:], *kv_loads, *smalls, q_load]:
        load.start()

    q2 = lax.div(ms, 2)
    pos = q2 + (ms - 2 * q2) * (n_seq - 1 - 2 * q2)

    def slot(p):
        p = lax.rem(p + 2 * n_seq, n_seq)
        back = lax.div(p, half)
        return (1 - back) * 2 * p + back * (2 * (n_seq - 1 - p) + 1)

    ends = (slot(pos + 1), slot(pos - 1))
    my = lax.div(mh, 2)
    mc = mh - 2 * my
    partner = {"head": 2 * my + 1 - mc}
    barrier = pltpu.get_barrier_semaphore()
    for end in ends:
        pl.semaphore_signal(barrier, inc=1, device_id={"seq": end}, device_id_type=MESH)
    for d in range(1, n_head):
        pl.semaphore_signal(
            barrier, inc=1, device_id={"head": lax.rem(mh + d, n_head)}, device_id_type=MESH
        )

    def spread(flat, row):
        for g in range(0, row.shape[1], HEAD_DIM):
            row[:, g : g + HEAD_DIM] = flat[g : g + HEAD_DIM].reshape(1, HEAD_DIM)

    m_ref[...] = jnp.full(m_ref.shape, LOW, F32)
    acc_ref[...] = jnp.zeros(acc_ref.shape, F32)
    ones = lax.broadcasted_iota(jnp.int32, (16, rows), 0)
    ones = jnp.where(ones == 0, 1.0, 0.0).astype(BF16)

    gain_load.wait()
    spread(gain_1d, gain_ref)
    block = 16

    def norm_quarter(q):
        for k in range(rows // 4 // block):
            at = pl.ds(q * (rows // 4) + k * block, block)
            x = tok[at, :].astype(F32)
            mean = jnp.sum(x * x, axis=1, keepdims=True) / width
            normed[at, :] = (x * lax.rsqrt(mean + EPS) * gain_ref[...]).astype(BF16)

    def rope(u, h=None):
        at = slice(None) if h is None else band(h)
        return u * cos[at, :] + pltpu.roll(u, HEAD_DIM // 2, 1) * sin[at, :]

    def project(h):
        kv = dot(normed[band(h), :], wkv[...])
        kbuf[ms, band(h)] = rope(kv[:, :HEAD_DIM] + kb_ref[...], h).astype(BF16)
        vbuf[ms, h] = jnp.transpose((kv[:, HEAD_DIM:] + vb_ref[...]).astype(BF16))

    def moved(way, turn, sub, kind, s, hops):
        at = slot(pos - hops if way == 0 else pos + hops)
        first, count = (way ^ turn) * part_rows, part_rows // SUBS
        if kind:
            part = vbuf.at[at, way ^ turn, pl.ds(sub * (HEAD_DIM // SUBS), HEAD_DIM // SUBS)]
        else:
            part = kbuf.at[at, pl.ds(first + sub * count, count)]
        unit = (((s - 1) * 2 + turn) * 2 + way) * 2 * SUBS + sub * 2 + kind
        return pltpu.make_async_remote_copy(
            src_ref=part,
            dst_ref=part,
            send_sem=ring_send.at[kind],
            recv_sem=ring_recv.at[unit],
            device_id={"seq": ends[way]},
            device_id_type=MESH,
        )

    def send(way, turn, sub, kind, s):
        return moved(way, turn, sub, kind, s, s - 1)

    def arrival(way, turn, sub, kind, s):
        return moved(way, turn, sub, kind, s, s)

    def send_own(way, turn):
        for kind in (0, 1):
            for sub in range(SUBS):
                send(way, turn, sub, kind, 1).start()

    def arrive(s, turn, kind):
        for sub in range(SUBS):
            for way in (0, 1):
                arrival(way, turn, sub, kind, s).wait_recv()

    def forward(s, turn):
        for kind in (0, 1):
            for sub in range(SUBS):
                for way in (0, 1):
                    arrival(way, turn, sub, kind, s).wait_recv()
                    send(way, turn, sub, kind, s + 1).start()

    for q in range(4):
        tok_loads[q].wait()
        norm_quarter(q)
    for small in smalls:
        small.wait()
    limit = length_ref[0]
    for flat, row in ((kb_1d, kb_ref), (vb_1d, vb_ref), (qb_1d, qb_ref), (fgain_1d, fgain_ref)):
        spread(flat, row)
    lane = lax.broadcasted_iota(jnp.int32, (1, HEAD_DIM), 1)
    sign = jnp.where(lane < HEAD_DIM // 2, -1.0, 1.0)
    co, so = far[0, :1], far[1, :1]
    cos[...] = near[0] * co - near[1] * so
    sin[...] = (near[1] * co + near[0] * so) * sign
    for load in kv_loads:
        load.wait()
    project(0)
    pl.semaphore_wait(barrier, n_head + 1)

    @pl.when(mc == 0)
    def _():
        send_own(0, 0)

    project(1)

    @pl.when(mc == 0)
    def _():
        send_own(1, 0)
        send_own(0, 1)
        send_own(1, 1)

    def put_query(h, u):
        u = rope(u + qb_ref[:, h * HEAD_DIM : (h + 1) * HEAD_DIM]) * HEAD_DIM ** (-0.5)
        qt[:, h * rows : (h + 1) * rows] = jnp.transpose(u.astype(BF16))

    def queries(first, last):
        u = dot(normed[...], wq[:, first * HEAD_DIM : last * HEAD_DIM])
        for h in range(first, last):
            put_query(h, u[:, (h - first) * HEAD_DIM : (h - first + 1) * HEAD_DIM])

    def attend(blocks, poll=None, last=False, group=1, values_in=None):
        row_at = lax.broadcasted_iota(jnp.int32, (part_rows, 1), 0)
        live = [
            jnp.concatenate([b * rows + h * part_rows + row_at for b, h in block], axis=0) < limit
            for block in blocks
        ]

        def keys(block):
            parts = [kbuf[b, h * part_rows : (h + 1) * part_rows] for b, h in block]
            return jnp.concatenate(parts, axis=0)

        def values(block):
            return jnp.concatenate([vbuf[b, h] for b, h in block], axis=1)

        def span(h):
            return slice(h * rows, min(h + group, heads) * rows)

        def scores(h):
            return [
                jnp.where(ok, dot(keys(block), qt[:, span(h)]), LOW)
                for block, ok in zip(blocks, live)
            ]

        def weigh(h, many):
            old = m_ref[:, span(h)][:1]
            top = functools.reduce(
                jnp.maximum, [jnp.max(s, axis=0, keepdims=True) for s in many], old
            )
            m_ref[:, span(h)] = jnp.broadcast_to(top, (8, top.shape[1]))
            return h, jnp.exp(old - top), [jnp.exp(s - top).astype(BF16) for s in many]

        def mix(h, alpha, weights):
            new = None
            for block, p in zip(blocks, weights):
                more = dot(jnp.concatenate([values(block), ones], axis=0), p)
                new = more if new is None else new + more
            new = acc_ref[:, span(h)] * alpha + new
            if last:
                done = (new[:HEAD_DIM] / new[HEAD_DIM : HEAD_DIM + 1]).astype(BF16)
                for g in range(done.shape[1] // rows):
                    at = slice((h + g) * HEAD_DIM, (h + g + 1) * HEAD_DIM)
                    att[:, at] = jnp.transpose(done[:, g * rows : (g + 1) * rows])
            else:
                acc_ref[:, span(h)] = new

        ready, held = scores(0), None
        for h in range(0, heads, group):
            after = scores(h + group) if h + group < heads else None
            weighed = weigh(h, ready)
            if h == 0 and values_in:
                values_in()
            if held is not None:
                mix(*held)
            held, ready = weighed, after
            if poll and h == heads // 2:
                poll()
        mix(*held)

    def whole(at):
        return ((at, 0), (at, 1))

    def pair(s):
        return [whole(slot(pos - s)), whole(slot(pos + s))]

    def cross_half(s, turn):
        return [((slot(pos - s), turn), (slot(pos + s), 1 - turn))]

    q_load.wait()
    o_load.start()
    queries(0, heads // 2)

    @pl.when(mc == 1)
    def _():
        for turn in (0, 1):
            for way in (0, 1):
                send_own(way, turn)

    queries(heads // 2, heads)
    forward(1, 0)
    attend([whole(ms)], group=GROUP)
    forward(1, 1)

    def ring_step(s, carry):
        attend(pair(s), lambda: forward(s + 1, 0))
        forward(s + 1, 1)
        return carry

    if half > 4:
        lax.fori_loop(1, half - 3, ring_step, 0)
    ring_step(half - 3, 0)
    attend(pair(half - 2), lambda: forward(half - 1, 0))
    arrive(half - 1, 1, 0)
    attend(pair(half - 1), values_in=lambda: arrive(half - 1, 1, 1))
    arrive(half, 0, 0)
    attend(
        cross_half(half, 0), last=True, group=GROUP, values_in=lambda: arrive(half, 0, 1)
    )
    o_load.wait()

    def far_y(d):
        return lax.rem(my + d, n_y)

    def partial(dest, at, wide):
        cols = pl.ds(pl.multiple_of(dest * share + at, HEAD_DIM), wide)
        return dot(att[...], wo[:, cols])

    def place(i):
        at, wide = chunks[i]
        return slice(at, at + wide)

    def pair_copy(i, d):
        return pltpu.make_async_remote_copy(
            src_ref=psend.at[d, :, place(i)],
            dst_ref=precv.at[d, :, place(i)],
            send_sem=pair_send.at[0],
            recv_sem=pair_recv.at[0 if d == 0 else i * (n_y - 1) + d],
            device_id=partner,
            device_id_type=MESH,
        )

    def cross_copy(i, d):
        return pltpu.make_async_remote_copy(
            src_ref=ysend.at[d - 1, :, place(i)],
            dst_ref=yrecv.at[d - 1, :, place(i)],
            send_sem=cross_send.at[0],
            recv_sem=cross_recv.at[i, d - 1],
            device_id={"head": 2 * far_y(d) + mc},
            device_id_type=MESH,
        )

    def part_sums(i, d):
        at, wide = chunks[i]
        psend[d, :, place(i)] = partial(2 * far_y(d) + 1 - mc, at, wide).astype(BF16)
        pair_copy(i, d).start()
        pown[d, :, place(i)] = partial(2 * far_y(d) + mc, at, wide)

    def across(i):
        for d in range(1, n_y):
            pair_copy(i, d).wait_recv()
            total = pown[d, :, place(i)] + precv[d, :, place(i)].astype(F32)
            ysend[d - 1, :, place(i)] = total.astype(BF16)
            cross_copy(i, d).start()

    @pl.when(mc == 0)
    def _():
        for i in range(len(chunks)):
            for d in range(1, n_y):
                part_sums(i, d)
            across(i)

    @pl.when(mc == 1)
    def _():
        for i in range(len(chunks)):
            for d in range(1, n_y):
                part_sums(i, d)
        for i in range(len(chunks)):
            across(i)

    for i in range(len(chunks)):
        part_sums(i, 0)

    squares = None
    pltpu.make_async_remote_copy(
        src_ref=psend.at[0],
        dst_ref=precv.at[0],
        send_sem=pair_send.at[0],
        recv_sem=pair_recv.at[0],
        device_id=partner,
        device_id_type=MESH,
    ).wait_recv()
    for i, (at, wide) in enumerate(chunks):
        mine = pl.ds(pl.multiple_of(mh * share + at, HEAD_DIM), wide)
        base = tok[:, mine].astype(F32) + (pown[0, :, place(i)] + precv[0, :, place(i)].astype(F32))
        for d in range(1, n_y):
            cross_copy(i, d).wait_recv()
            base = base + yrecv[d - 1, :, place(i)].astype(F32)
        hid[:, at : at + wide] = base
        hid_bf[:, at : at + wide] = base.astype(BF16)
        for g in range(0, wide, HEAD_DIM):
            piece = base[:, g : g + HEAD_DIM]
            squares = piece * piece if squares is None else squares + piece * piece

    def exchange(buf, axis, me, n, sems):
        def copy(d, slot_at):
            return pltpu.make_async_remote_copy(
                src_ref=buf.at[slot_at],
                dst_ref=buf.at[slot_at],
                send_sem=sems.at[0],
                recv_sem=sems.at[1],
                device_id={axis: lax.rem(me + d, n)},
                device_id_type=MESH,
            )

        for d in range(n - 1, 0, -1):
            copy(d, me).start()
        part = buf.at[pl.ds(0, n - 1)]
        pltpu.make_async_remote_copy(
            src_ref=part,
            dst_ref=part,
            send_sem=sems.at[0],
            recv_sem=sems.at[1],
            device_id=partner,
            device_id_type=MESH,
        ).wait_recv()

    def head_sum(buf, sems, value):
        buf[mh] = jnp.broadcast_to(value, buf.shape[1:])
        exchange(buf, "head", mh, n_head, sems)
        return functools.reduce(lambda a, b: a + b, [buf[d][:1] for d in range(n_head)])

    square_row = jnp.sum(jnp.transpose(squares), axis=0, keepdims=True)
    power = head_sum(sqbuf, sq_sem, square_row)
    where = ms * rows + lax.broadcasted_iota(jnp.int32, (1, rows), 1)
    scale = jnp.where(where < limit, lax.rsqrt(power / width + EPS), 0.0)
    scale = jnp.transpose(jnp.broadcast_to(scale, (HEAD_DIM, rows)))

    groups = pbuf.shape[1]
    sums = []
    for g in range(0, share, HEAD_DIM):
        at = slice(g, g + HEAD_DIM)
        sums.append(jnp.sum(hid[:, at] * scale, axis=0, keepdims=True) * fgain_ref[:, at])
    sums += [jnp.zeros((1, HEAD_DIM), F32)] * (groups - len(sums))
    pbuf[ms] = jnp.concatenate(sums, axis=0)

    shared[...] = pbuf[ms].astype(BF16)

    def share_copy(d):
        return pltpu.make_async_remote_copy(
            src_ref=shared,
            dst_ref=other.at[ms],
            send_sem=share_sem.at[0],
            recv_sem=share_sem.at[1],
            device_id={"seq": lax.rem(ms + d, n_seq), **partner},
            device_id_type=MESH,
        )

    for d in range(n_seq - 1, -1, -1):
        share_copy(d).start()
    exchange(pbuf, "seq", ms, n_seq, pool_sem)
    every_share = pltpu.make_async_remote_copy(
        src_ref=other,
        dst_ref=other,
        send_sem=share_sem.at[0],
        recv_sem=share_sem.at[1],
        device_id=partner,
        device_id_type=MESH,
    )
    every_share.wait_recv()
    mean = functools.reduce(lambda a, b: a + b, [pbuf[d] for d in range(n_seq)])
    mean = mean / limit.astype(F32)
    near_mean = functools.reduce(
        lambda a, b: a + b, [other[d].astype(F32) for d in range(n_seq)]
    )
    near_mean = near_mean / limit.astype(F32)
    power = jnp.sum(mean * mean + near_mean * near_mean, axis=0, keepdims=True)
    wbuf[my] = jnp.broadcast_to(power, wbuf.shape[1:])

    @pl.when(mc == 1)
    def _():
        for d in range(1, n_y):
            for c in (0, 1):
                pltpu.make_async_remote_copy(
                    src_ref=wbuf.at[my],
                    dst_ref=wbuf.at[my],
                    send_sem=pow_sem.at[0],
                    recv_sem=pow_sem.at[1],
                    device_id={"head": 2 * far_y(d) + c},
                    device_id_type=MESH,
                ).start()

    part = wbuf.at[pl.ds(0, n_y - 1)]
    pltpu.make_async_remote_copy(
        src_ref=part,
        dst_ref=part,
        send_sem=pow_sem.at[0],
        recv_sem=pow_sem.at[1],
        device_id=partner,
        device_id_type=MESH,
    ).wait_recv()
    total = functools.reduce(lambda a, b: a + b, [wbuf[y][:1] for y in range(n_y)])
    pooled = mean * lax.rsqrt(jnp.sum(total, axis=1, keepdims=True) / width + EPS)
    for g in range(share // HEAD_DIM):
        emb_ref[g * HEAD_DIM : (g + 1) * HEAD_DIM] = pooled[g : g + 1].reshape(HEAD_DIM)

    def all_sent(ref, sems, n):
        part = ref.at[pl.ds(0, n)]
        pltpu.make_async_remote_copy(
            src_ref=part,
            dst_ref=part,
            send_sem=sems.at[0],
            recv_sem=sems.at[0],
            device_id=partner,
            device_id_type=MESH,
        ).wait_send()

    all_sent(kbuf, ring_send.at[pl.ds(0, 1)], n_seq - 1)
    all_sent(vbuf, ring_send.at[pl.ds(1, 1)], n_seq - 1)
    all_sent(psend, pair_send, n_y)
    all_sent(ysend, cross_send, n_y - 1)
    all_sent(sqbuf, sq_sem, n_head - 1)
    all_sent(pbuf, pool_sem, n_seq - 1)
    every_share.wait_send()

    @pl.when(mc == 1)
    def _():
        all_sent(wbuf, pow_sem, 2 * (n_y - 1))


def write_out(hidden_ref, emb_ref, hidden_hbm, emb_hbm, sems):
    copies = [
        pltpu.make_async_copy(hidden_ref, hidden_hbm, sems.at[0]),
        pltpu.make_async_copy(emb_ref, emb_hbm, sems.at[1]),
    ]
    for copy in copies:
        copy.start()
    for copy in copies:
        copy.wait()


def body(
    n_seq,
    n_head,
    tokens,
    length,
    in_gain,
    q_weight,
    q_bias,
    k_weight,
    k_bias,
    v_weight,
    v_bias,
    o_weight,
    final_gain,
):
    rows, width = tokens.shape
    share = width // n_head
    heads = q_weight.shape[1] // HEAD_DIM
    half = n_seq // 2
    n_y = n_head // 2
    inverse = ROPE_BASE ** (-(np.arange(HEAD_DIM // 2) * 2.0) / HEAD_DIM)
    inverse = np.concatenate([inverse, inverse])[None, :]
    near = np.arange(rows)[:, None] * inverse
    near = np.stack([np.cos(near), np.sin(near)]).astype(np.float32)
    far = (np.arange(n_seq) * rows)[:, None] * inverse
    far = np.stack([np.cos(far), np.sin(far)], axis=1).astype(np.float32)
    far = np.repeat(far[:, :, None, :], 8, axis=2)

    chunks = widths(share)
    groups = -(-share // (8 * HEAD_DIM)) * 8
    dma = pltpu.SemaphoreType.DMA
    hbm = pl.BlockSpec(memory_space=pltpu.HBM)
    vmem = pl.BlockSpec(memory_space=pltpu.VMEM)
    shapes = (
        jax.ShapeDtypeStruct((rows, share), BF16),
        jax.ShapeDtypeStruct((share,), F32),
    )
    operands = (
        length,
        tokens,
        in_gain,
        q_weight,
        q_bias,
        k_weight,
        k_bias,
        v_weight,
        v_bias,
        o_weight,
        final_gain,
        jnp.asarray(near),
        jnp.asarray(far),
    )
    hidden, embedding = pl.pallas_call(
        functools.partial(kernel, n_seq, n_head),
        out_shape=shapes,
        in_specs=[hbm] * 13,
        out_specs=(vmem, vmem),
        scratch_shapes=[
            pltpu.SMEM((1,), jnp.int32),
            pltpu.VMEM((width,), F32),
            pltpu.VMEM((heads * HEAD_DIM,), F32),
            pltpu.VMEM((HEAD_DIM,), F32),
            pltpu.VMEM((HEAD_DIM,), F32),
            pltpu.VMEM((share,), F32),
            pltpu.VMEM(near.shape, F32),
            pltpu.VMEM(far.shape[1:], F32),
            pltpu.VMEM((1, width), F32),
            pltpu.VMEM((1, heads * HEAD_DIM), F32),
            pltpu.VMEM((1, HEAD_DIM), F32),
            pltpu.VMEM((1, HEAD_DIM), F32),
            pltpu.VMEM((1, share), F32),
            pltpu.VMEM((rows, width), BF16),
            pltpu.VMEM((rows, width), BF16),
            pltpu.VMEM((width, 2 * HEAD_DIM), BF16),
            pltpu.VMEM(q_weight.shape, BF16),
            pltpu.VMEM(o_weight.shape, BF16),
            pltpu.VMEM((rows, HEAD_DIM), F32),
            pltpu.VMEM((rows, HEAD_DIM), F32),
            pltpu.VMEM((HEAD_DIM, heads * rows), BF16),
            pltpu.VMEM((n_seq, rows, HEAD_DIM), BF16),
            pltpu.VMEM((n_seq, 2, HEAD_DIM, rows // 2), BF16),
            pltpu.VMEM((8, heads * rows), F32),
            pltpu.VMEM((HEAD_DIM + 16, heads * rows), F32),
            pltpu.VMEM((rows, heads * HEAD_DIM), BF16),
            pltpu.VMEM((rows, share), F32),
            pltpu.VMEM((n_y, rows, share), BF16),
            pltpu.VMEM((n_y, rows, share), BF16),
            pltpu.VMEM((n_y, rows, share), F32),
            pltpu.VMEM((n_y - 1, rows, share), BF16),
            pltpu.VMEM((n_y - 1, rows, share), BF16),
            pltpu.VMEM((n_head, 8, rows), F32),
            pltpu.VMEM((n_seq, groups, HEAD_DIM), F32),
            pltpu.VMEM((n_head, 8, HEAD_DIM), F32),
            pltpu.VMEM((groups, HEAD_DIM), BF16),
            pltpu.VMEM((n_seq, groups, HEAD_DIM), BF16),
            dma((16,)),
            dma((2,)),
            dma((SUBS * (8 * half - 4),)),
            dma((1,)),
            dma((1 + len(chunks) * (n_y - 1),)),
            dma((1,)),
            dma((len(chunks), n_y - 1)),
            dma((2,)),
            dma((2,)),
            dma((2,)),
            dma((2,)),
        ],
        compiler_params=pltpu.CompilerParams(
            collective_id=0, has_side_effects=True, vmem_limit_bytes=48 * 1024 * 1024
        ),
    )(operands[0], *[pltpu.with_memory_space_constraint(x, pltpu.HBM) for x in operands[1:]])
    return pl.pallas_call(
        write_out,
        out_shape=shapes,
        in_specs=[vmem, vmem],
        out_specs=(hbm, hbm),
        scratch_shapes=[dma((2,))],
        compiler_params=pltpu.CompilerParams(vmem_limit_bytes=2 * 1024 * 1024),
    )(hidden, embedding)


def solution(mesh):
    in_specs = (
        P("seq", None),
        P(),
        P(),
        P(None, "head"),
        P("head"),
        P(None, "head"),
        P("head"),
        P(None, "head"),
        P("head"),
        P("head", None),
        P("head"),
    )
    out_specs = (P("seq", "head"), P("head"))
    step = functools.partial(body, mesh.shape["seq"], mesh.shape["head"])
    return jax.shard_map(step, mesh=mesh, in_specs=in_specs, out_specs=out_specs, check_vma=False)
```
